8 devices in a mesh: dp: 1 (over z), x: 8 (over y, x, core).
Axes of the slice: x: 2, y: 2, z: 1, core: 2. Of those that a mesh axis runs over, the one named last changes fastest.
Arguments:
- start_pos: int32 [256], P('dp')
- hidden_in: bfloat16 [4, 256, 5120], P(None, ('dp', 'x'))
- k_cache: bfloat16 [256, 256, 8, 128], P('dp', None, 'x')
- v_cache: bfloat16 [256, 256, 8, 128], P('dp', None, 'x')
- attn_norm: bfloat16 [5120], replicated
- w_q: bfloat16 [5120, 5120], replicated
- w_k: bfloat16 [5120, 1024], replicated
- w_v: bfloat16 [5120, 1024], replicated
- q_norm: bfloat16 [128], replicated
- k_norm: bfloat16 [128], replicated
- w_o: bfloat16 [5120, 5120], replicated
- mlp_norm: bfloat16 [5120], replicated
- w_gate: bfloat16 [5120, 17408], replicated
- w_up: bfloat16 [5120, 17408], replicated
- w_down: bfloat16 [17408, 5120], replicated
Outputs:
- output 1: bfloat16 [4, 256, 5120], P(None, ('dp', 'x'))
- output 2: bfloat16 [256, 256, 8, 128], P(('dp', 'x'))
- output 3: bfloat16 [256, 256, 8, 128], P(('dp', 'x'))
All inputs are finite; a program needn't handle non-finite values.
Results may differ from the reference program's by a relative error of at most 0.0104501.
Values are sent between devices in bfloat16 or wider.
A program may use at most 2.75 GiB of HBM per device.

```python
import math
import jax
import jax.numpy as jnp
from jax import lax

BATCH = 256
T = 256
D = 5120
HEADS = 40
KV_HEADS = 8
HEAD = 128
FF = 17408
STEPS = 4

EPS = 1e-6
THETA = 1000000.0
Q_GAIN = math.sqrt(0.8 * math.log(T))
K_GAIN = math.sqrt(2.0 * math.log(T))


def rms_norm(values, gain_vec):
    values32 = values.astype(jnp.float32)
    inv_rms = lax.rsqrt(jnp.mean(values32 * values32, axis=-1, keepdims=True) + EPS)
    return values32 * inv_rms * gain_vec.astype(jnp.float32)


def rotary(values, positions):
    half_dim = HEAD // 2
    inv_freq = jnp.power(THETA, -jnp.arange(half_dim, dtype=jnp.float32) * 2.0 / HEAD)
    angles = positions.astype(jnp.float32)[..., None, None] * inv_freq
    cos_part = jnp.cos(angles)
    sin_part = jnp.sin(angles)
    first_half = values[..., :half_dim]
    second_half = values[..., half_dim:]
    return jnp.concatenate([first_half * cos_part - second_half * sin_part, second_half * cos_part + first_half * sin_part], axis=-1)


def setup_inputs(seed: int = 0, part: int = 0) -> dict:
    base_keys = jax.random.split(jax.random.key(seed), 16)

    def part_normal(index, shape):
        return jax.random.normal(jax.random.fold_in(base_keys[index], part), shape, jnp.float32)

    def shared_normal(index, shape):
        return jax.random.normal(base_keys[index], shape, jnp.float32)

    pos_key = jax.random.fold_in(base_keys[0], part)
    pos_draw = jax.random.randint(jax.random.fold_in(pos_key, 1), (BATCH,), T // 4, T - 3)
    top_row = jax.random.randint(jax.random.fold_in(pos_key, 2), (), 0, BATCH)
    start_pos = jnp.where(jnp.arange(BATCH) == top_row, T - 4, pos_draw).astype(jnp.int32)
    return dict(
        start_pos=start_pos,
        hidden_in=part_normal(1, (STEPS, BATCH, D)).astype(jnp.bfloat16),
        k_cache=part_normal(2, (BATCH, T, KV_HEADS, HEAD)).astype(jnp.bfloat16),
        v_cache=part_normal(3, (BATCH, T, KV_HEADS, HEAD)).astype(jnp.bfloat16),
        attn_norm=(1.0 + 0.2 * shared_normal(4, (D,))).astype(jnp.bfloat16),
        w_q=(shared_normal(5, (D, HEADS * HEAD)) * D ** -0.5).astype(jnp.bfloat16),
        w_k=(shared_normal(6, (D, KV_HEADS * HEAD)) * D ** -0.5).astype(jnp.bfloat16),
        w_v=(shared_normal(7, (D, KV_HEADS * HEAD)) * D ** -0.5).astype(jnp.bfloat16),
        q_norm=(Q_GAIN * (1.0 + 0.2 * shared_normal(8, (HEAD,)))).astype(jnp.bfloat16),
        k_norm=(K_GAIN * (1.0 + 0.2 * shared_normal(9, (HEAD,)))).astype(jnp.bfloat16),
        w_o=(shared_normal(10, (HEADS * HEAD, D)) * (HEADS * HEAD) ** -0.5).astype(jnp.bfloat16),
        mlp_norm=(1.0 + 0.2 * shared_normal(11, (D,))).astype(jnp.bfloat16),
        w_gate=(shared_normal(12, (D, FF)) * D ** -0.5).astype(jnp.bfloat16),
        w_up=(shared_normal(13, (D, FF)) * D ** -0.5).astype(jnp.bfloat16),
        w_down=(shared_normal(14, (FF, D)) * FF ** -0.5).astype(jnp.bfloat16),
    )


def reference(start_pos, hidden_in, k_cache, v_cache, attn_norm, w_q, w_k, w_v, q_norm, k_norm, w_o, mlp_norm, w_gate, w_up, w_down):
    group_size = HEADS // KV_HEADS
    score_scale = HEAD ** -0.5
    tokens = rms_norm(hidden_in, attn_norm).astype(jnp.bfloat16).reshape(STEPS * BATCH, D)
    queries = jnp.dot(tokens, w_q, preferred_element_type=jnp.float32).reshape(STEPS, BATCH, HEADS, HEAD)
    keys_new = jnp.dot(tokens, w_k, preferred_element_type=jnp.float32).reshape(STEPS, BATCH, KV_HEADS, HEAD)
    values_new = jnp.dot(tokens, w_v, preferred_element_type=jnp.float32).reshape(STEPS, BATCH, KV_HEADS, HEAD)
    positions = start_pos[None, :] + jnp.arange(STEPS)[:, None]
    queries = rotary(rms_norm(queries, q_norm), positions).astype(jnp.bfloat16)
    keys_new = rotary(rms_norm(keys_new, k_norm), positions).astype(jnp.bfloat16)
    values_new = values_new.astype(jnp.bfloat16)

    def one_row(row_inputs):
        row_q, row_k, row_v, row_kc, row_vc, row_pos = row_inputs

        def one_step(carry_in, step_inputs):
            cache_k, cache_v = carry_in
            step_q, step_k, step_v, slot_idx = step_inputs
            cache_k = lax.dynamic_update_slice(cache_k, step_k[None], (slot_idx, 0, 0))
            cache_v = lax.dynamic_update_slice(cache_v, step_v[None], (slot_idx, 0, 0))
            grouped = step_q.reshape(KV_HEADS, group_size, HEAD).astype(jnp.float32)
            scores = jnp.einsum('kgd,tkd->kgt', grouped, cache_k.astype(jnp.float32)) * score_scale
            slot_valid = jnp.arange(T) <= slot_idx
            scores = jnp.where(slot_valid, scores, -jnp.inf)
            weights = jnp.exp(scores - jnp.max(scores, axis=-1, keepdims=True))
            weight_sum = jnp.sum(weights, axis=-1)
            mixed_vals = jnp.einsum('kgt,tkd->kgd', weights.astype(jnp.bfloat16).astype(jnp.float32), cache_v.astype(jnp.float32))
            attended = (mixed_vals / weight_sum[..., None]).astype(jnp.bfloat16).reshape(HEADS * HEAD)
            return (cache_k, cache_v), attended

        (final_k, final_v), step_outs = lax.scan(one_step, (row_kc, row_vc), (row_q, row_k, row_v, row_pos + jnp.arange(STEPS)))
        return step_outs, final_k, final_v

    row_outs, k_out, v_out = lax.map(one_row, (jnp.swapaxes(queries, 0, 1), jnp.swapaxes(keys_new, 0, 1), jnp.swapaxes(values_new, 0, 1), k_cache, v_cache, start_pos))
    attended = jnp.swapaxes(row_outs, 0, 1).reshape(STEPS * BATCH, HEADS * HEAD)
    attn_out = jnp.dot(attended, w_o, preferred_element_type=jnp.float32).reshape(STEPS, BATCH, D)
    residual = (hidden_in.astype(jnp.float32) + attn_out).astype(jnp.bfloat16)
    normed = rms_norm(residual, mlp_norm).astype(jnp.bfloat16).reshape(STEPS * BATCH, D)
    gate_val = jnp.dot(normed, w_gate, preferred_element_type=jnp.float32)
    up_val = jnp.dot(normed, w_up, preferred_element_type=jnp.float32)
    activated = (jax.nn.silu(gate_val) * up_val).astype(jnp.bfloat16)
    down_val = jnp.dot(activated, w_down, preferred_element_type=jnp.float32).reshape(STEPS, BATCH, D)
    out_hidden = (residual.astype(jnp.float32) + down_val).astype(jnp.bfloat16)
    return (out_hidden, k_out, v_out)
```

```python
import jax
import jax.numpy as jnp
from jax import lax
from jax.experimental import pallas as pl
from jax.experimental.pallas import tpu as pltpu
from jax.sharding import PartitionSpec as P

EPS = 1e-6
THETA = 1000000.0


def rms_norm(values, gain_vec):
    values32 = values.astype(jnp.float32)
    inv_rms = lax.rsqrt(jnp.mean(values32 * values32, axis=-1, keepdims=True) + EPS)
    return values32 * inv_rms * gain_vec.astype(jnp.float32)


def rotary(values, positions):
    head_dim = values.shape[-1]
    half_dim = head_dim // 2
    inv_freq = jnp.power(THETA, -jnp.arange(half_dim, dtype=jnp.float32) * 2.0 / head_dim)
    angles = positions.astype(jnp.float32)[..., None, None] * inv_freq
    cos_part = jnp.cos(angles)
    sin_part = jnp.sin(angles)
    first_half = values[..., :half_dim]
    second_half = values[..., half_dim:]
    return jnp.concatenate([first_half * cos_part - second_half * sin_part, second_half * cos_part + first_half * sin_part], axis=-1)


def project(hidden, positions, attn_norm, w_q, w_k, w_v, q_norm, k_norm):
    n_steps, num_rows = hidden.shape[0], hidden.shape[1]
    head_dim = q_norm.shape[0]
    normed = rms_norm(hidden, attn_norm).astype(jnp.bfloat16)
    queries = jnp.einsum('sbd,de->sbe', normed, w_q, preferred_element_type=jnp.float32).reshape(n_steps, num_rows, -1, head_dim)
    keys_new = jnp.einsum('sbd,de->sbe', normed, w_k, preferred_element_type=jnp.float32).reshape(n_steps, num_rows, -1, head_dim)
    values_new = jnp.einsum('sbd,de->sbe', normed, w_v, preferred_element_type=jnp.float32).reshape(n_steps, num_rows, -1, head_dim)
    queries = rotary(rms_norm(queries, q_norm), positions).astype(jnp.bfloat16)
    keys_new = rotary(rms_norm(keys_new, k_norm), positions).astype(jnp.bfloat16)
    return queries, keys_new, values_new.astype(jnp.bfloat16)


def attend(queries, cache_k, cache_v, keys_new, values_new, start_pos):
    n_steps, num_rows, n_heads, head_dim = queries.shape
    num_slots, kv_local = cache_k.shape[1], cache_k.shape[2]
    grouped = queries.reshape(n_steps, num_rows, kv_local, n_heads // kv_local, head_dim)
    score_scale = head_dim ** -0.5
    old_scores = jnp.einsum('sbkgd,btkd->bkgst', grouped, cache_k, preferred_element_type=jnp.float32) * score_scale
    old_valid = (jnp.arange(num_slots)[None, :] < start_pos[:, None])[:, None, None, None, :]
    old_scores = jnp.where(old_valid, old_scores, -jnp.inf)
    new_scores = jnp.einsum('sbkgd,jbkd->bkgsj', grouped, keys_new, preferred_element_type=jnp.float32) * score_scale
    new_valid = jnp.arange(n_steps)[:, None] >= jnp.arange(n_steps)[None, :]
    new_scores = jnp.where(new_valid, new_scores, -jnp.inf)
    peak_score = jnp.maximum(jnp.max(old_scores, axis=-1, keepdims=True), jnp.max(new_scores, axis=-1, keepdims=True))
    old_weights = jnp.exp(old_scores - peak_score)
    new_weights = jnp.exp(new_scores - peak_score)
    weight_sum = jnp.sum(old_weights, axis=-1) + jnp.sum(new_weights, axis=-1)
    mixed_vals = jnp.einsum('bkgst,btkd->sbkgd', old_weights.astype(jnp.bfloat16), cache_v, preferred_element_type=jnp.float32)
    mixed_vals = mixed_vals + jnp.einsum('bkgsj,jbkd->sbkgd', new_weights.astype(jnp.bfloat16), values_new, preferred_element_type=jnp.float32)
    mixed_vals = mixed_vals / jnp.transpose(weight_sum, (3, 0, 1, 2))[..., None]
    return mixed_vals.astype(jnp.bfloat16).reshape(n_steps, num_rows, n_heads, head_dim)


def finish(hidden, attended, w_o, mlp_norm, w_gate, w_up, w_down):
    n_steps, num_rows = attended.shape[0], attended.shape[1]
    flat_attn = attended.reshape(n_steps, num_rows, -1)
    attn_out = jnp.einsum('sbe,ed->sbd', flat_attn, w_o, preferred_element_type=jnp.float32)
    residual = (hidden.astype(jnp.float32) + attn_out).astype(jnp.bfloat16)
    normed = rms_norm(residual, mlp_norm).astype(jnp.bfloat16)
    gate_val = jnp.einsum('sbd,df->sbf', normed, w_gate, preferred_element_type=jnp.float32)
    up_val = jnp.einsum('sbd,df->sbf', normed, w_up, preferred_element_type=jnp.float32)
    activated = (jax.nn.silu(gate_val) * up_val).astype(jnp.bfloat16)
    down_val = jnp.einsum('sbf,fd->sbd', activated, w_down, preferred_element_type=jnp.float32)
    return (residual.astype(jnp.float32) + down_val).astype(jnp.bfloat16)


def merge_kernel(pos_ref, blocks_ref, fresh_ref, out_ref, wide_ref):
    num_heads = blocks_ref.shape[0]
    for head_idx in range(num_heads):
        wide_ref[:, head_idx, :] = blocks_ref[head_idx, 0].astype(jnp.float32)
    out_ref[0] = wide_ref[...].astype(out_ref.dtype)
    first_slot = pos_ref[pl.program_id(0)]
    for step_idx in range(fresh_ref.shape[0]):
        out_ref[0, first_slot + step_idx] = fresh_ref[step_idx, 0]


def merge_heads(blocks, fresh_rows, start_pos):
    num_heads, num_rows, num_slots, head_dim = blocks.shape
    n_steps = fresh_rows.shape[0]
    return pl.pallas_call(
        merge_kernel,
        out_shape=jax.ShapeDtypeStruct((num_rows, num_slots, num_heads, head_dim), blocks.dtype),
        grid_spec=pltpu.PrefetchScalarGridSpec(
            num_scalar_prefetch=1,
            grid=(num_rows,),
            in_specs=[
                pl.BlockSpec((num_heads, 1, num_slots, head_dim), lambda b, pos: (0, b, 0, 0)),
                pl.BlockSpec((n_steps, 1, num_heads, head_dim), lambda b, pos: (0, b, 0, 0)),
            ],
            out_specs=pl.BlockSpec((1, num_slots, num_heads, head_dim), lambda b, pos: (b, 0, 0, 0)),
            scratch_shapes=[pltpu.VMEM((num_slots, num_heads, head_dim), jnp.float32)],
        ),
        cost_estimate=pl.CostEstimate(flops=10**9, bytes_accessed=2 * blocks.size * 2, transcendentals=0),
    )(start_pos, blocks, fresh_rows)


def solution(mesh):
    n_dev = mesh.shape['x']
    row_spec = P(None, ('dp', 'x'), None)
    cache_in = P('dp', None, 'x', None)
    cache_out = P(('dp', 'x'), None, None, None)

    def swap(arr):
        return lax.all_to_all(arr, 'x', 0, 0, tiled=True)

    def local_run(start_pos, hidden_in, k_heads, v_heads, attn_norm, w_q, w_k, w_v, q_norm, k_norm, w_o, mlp_norm, w_gate, w_up, w_down):
        n_steps, num_rows, _ = hidden_in.shape
        all_rows, num_slots, _, head_dim = k_heads.shape
        my_pos = lax.dynamic_slice_in_dim(start_pos, lax.axis_index('x') * num_rows, num_rows)
        k_own, v_own = k_heads[:, :, 0], v_heads[:, :, 0]
        k_got = swap(k_own).reshape(n_dev, num_rows, num_slots, head_dim)
        positions = my_pos[None, :] + jnp.arange(n_steps)[:, None]
        queries, keys_new, values_new = project(hidden_in, positions, attn_norm, w_q, w_k, w_v, q_norm, k_norm)
        group = queries.shape[2] // n_dev
        q_send = queries.reshape(n_steps, num_rows, n_dev, group, head_dim).transpose(2, 0, 3, 1, 4).reshape(n_dev, n_steps * group, num_rows, head_dim)
        k_send = keys_new.transpose(2, 0, 1, 3)
        v_send = values_new.transpose(2, 0, 1, 3)
        sent = jnp.concatenate([q_send, k_send, v_send], axis=1)
        got = swap(sent)
        got = got.transpose(1, 0, 2, 3).reshape(n_steps * (group + 2), all_rows, head_dim)
        q_got = got[:n_steps * group].reshape(n_steps, group, all_rows, head_dim).transpose(0, 2, 1, 3)
        kn_got = got[n_steps * group:n_steps * (group + 1), :, None]
        vn_got = got[n_steps * (group + 1):, :, None]
        mixed = attend(q_got, k_heads, v_heads, kn_got, vn_got, start_pos)
        mixed = mixed.reshape(n_steps, n_dev, num_rows, group, head_dim).transpose(1, 0, 3, 2, 4)
        v_got = swap(v_own).reshape(n_dev, num_rows, num_slots, head_dim)
        back = swap(mixed)
        attended = back.transpose(1, 3, 0, 2, 4).reshape(n_steps, num_rows, n_dev * group, head_dim)
        out_hidden = finish(hidden_in, attended, w_o, mlp_norm, w_gate, w_up, w_down)
        k_out = merge_heads(k_got, keys_new, my_pos)
        v_out = merge_heads(v_got, values_new, my_pos)
        return out_hidden, k_out, v_out

    return jax.shard_map(local_run, mesh=mesh, in_specs=(P('dp'), row_spec, cache_in, cache_in) + (P(),) * 11, out_specs=(row_spec, cache_out, cache_out), check_vma=False)
```

```python
import functools

import jax
import jax.numpy as jnp
from jax import lax
from jax.experimental import pallas as pl
from jax.experimental.pallas import tpu as pltpu
from jax.sharding import PartitionSpec as P

EPS = 1e-6
THETA = 1000000.0


def rms_norm(values, gain_vec):
    values32 = values.astype(jnp.float32)
    inv_rms = lax.rsqrt(jnp.mean(values32 * values32, axis=-1, keepdims=True) + EPS)
    return values32 * inv_rms * gain_vec.astype(jnp.float32)


def rotary(values, positions):
    head_dim = values.shape[-1]
    half_dim = head_dim // 2
    inv_freq = jnp.power(THETA, -jnp.arange(half_dim, dtype=jnp.float32) * 2.0 / head_dim)
    angles = positions.astype(jnp.float32)[..., None, None] * inv_freq
    cos_part = jnp.cos(angles)
    sin_part = jnp.sin(angles)
    first_half = values[..., :half_dim]
    second_half = values[..., half_dim:]
    return jnp.concatenate([first_half * cos_part - second_half * sin_part, second_half * cos_part + first_half * sin_part], axis=-1)


def project(hidden, positions, attn_norm, w_q, w_k, w_v, q_norm, k_norm):
    n_steps, num_rows = hidden.shape[0], hidden.shape[1]
    head_dim = q_norm.shape[0]
    normed = rms_norm(hidden, attn_norm).astype(jnp.bfloat16)
    queries = jnp.einsum('sbd,de->sbe', normed, w_q, preferred_element_type=jnp.float32).reshape(n_steps, num_rows, -1, head_dim)
    keys_new = jnp.einsum('sbd,de->sbe', normed, w_k, preferred_element_type=jnp.float32).reshape(n_steps, num_rows, -1, head_dim)
    values_new = jnp.einsum('sbd,de->sbe', normed, w_v, preferred_element_type=jnp.float32).reshape(n_steps, num_rows, -1, head_dim)
    queries = rotary(rms_norm(queries, q_norm), positions).astype(jnp.bfloat16)
    keys_new = rotary(rms_norm(keys_new, k_norm), positions).astype(jnp.bfloat16)
    return queries, keys_new, values_new.astype(jnp.bfloat16)


def attend(queries, cache_k, cache_v, keys_new, values_new, start_pos):
    n_steps, num_rows, n_heads, head_dim = queries.shape
    num_slots, kv_local = cache_k.shape[1], cache_k.shape[2]
    grouped = queries.reshape(n_steps, num_rows, kv_local, n_heads // kv_local, head_dim)
    score_scale = head_dim ** -0.5
    old_scores = jnp.einsum('sbkgd,btkd->bkgst', grouped, cache_k, preferred_element_type=jnp.float32) * score_scale
    old_valid = (jnp.arange(num_slots)[None, :] < start_pos[:, None])[:, None, None, None, :]
    old_scores = jnp.where(old_valid, old_scores, -jnp.inf)
    new_scores = jnp.einsum('sbkgd,jbkd->bkgsj', grouped, keys_new, preferred_element_type=jnp.float32) * score_scale
    new_valid = jnp.arange(n_steps)[:, None] >= jnp.arange(n_steps)[None, :]
    new_scores = jnp.where(new_valid, new_scores, -jnp.inf)
    peak_score = jnp.maximum(jnp.max(old_scores, axis=-1, keepdims=True), jnp.max(new_scores, axis=-1, keepdims=True))
    old_weights = jnp.exp(old_scores - peak_score)
    new_weights = jnp.exp(new_scores - peak_score)
    weight_sum = jnp.sum(old_weights, axis=-1) + jnp.sum(new_weights, axis=-1)
    mixed_vals = jnp.einsum('bkgst,btkd->sbkgd', old_weights.astype(jnp.bfloat16), cache_v, preferred_element_type=jnp.float32)
    mixed_vals = mixed_vals + jnp.einsum('bkgsj,jbkd->sbkgd', new_weights.astype(jnp.bfloat16), values_new, preferred_element_type=jnp.float32)
    mixed_vals = mixed_vals / jnp.transpose(weight_sum, (3, 0, 1, 2))[..., None]
    return mixed_vals.astype(jnp.bfloat16).reshape(n_steps, num_rows, n_heads, head_dim)


def finish(hidden, attended, w_o, mlp_norm, w_gate, w_up, w_down):
    n_steps, num_rows = attended.shape[0], attended.shape[1]
    flat_attn = attended.reshape(n_steps, num_rows, -1)
    attn_out = jnp.einsum('sbe,ed->sbd', flat_attn, w_o, preferred_element_type=jnp.float32)
    residual = (hidden.astype(jnp.float32) + attn_out).astype(jnp.bfloat16)
    normed = rms_norm(residual, mlp_norm).astype(jnp.bfloat16)
    gate_val = jnp.einsum('sbd,df->sbf', normed, w_gate, preferred_element_type=jnp.float32)
    up_val = jnp.einsum('sbd,df->sbf', normed, w_up, preferred_element_type=jnp.float32)
    activated = (jax.nn.silu(gate_val) * up_val).astype(jnp.bfloat16)
    down_val = jnp.einsum('sbf,fd->sbd', activated, w_down, preferred_element_type=jnp.float32)
    return (residual.astype(jnp.float32) + down_val).astype(jnp.bfloat16)


ROW_PAD = 9
K_CUTS, V_CUTS = (8, 20, 32), (14, 26, 32)
SWAP_ORDER = (2, 4, 3, 5, 6, 7, 1)


def cuts(num_rows, ends):
    ends = [num_rows * e // 32 for e in ends]
    return [(lo, hi - lo) for lo, hi in zip([0] + ends[:-1], ends)]


def merge_kernel(row_base, meta_ref, *refs):
    n_dev = (len(refs) - 4) if len(refs) > 11 else (len(refs) - 3)
    block_refs, fresh_ref = refs[:n_dev], refs[n_dev]
    out_ref, wide_ref = refs[-2], refs[-1]
    num_slots = out_ref.shape[1]
    for rel_idx in range(n_dev):
        head_idx = meta_ref[rel_idx]
        wide_ref[pl.ds(head_idx, num_slots, stride=ROW_PAD), :] = block_refs[rel_idx][0].astype(jnp.float32)
    for slot_idx in range(num_slots):
        out_ref[0, slot_idx] = wide_ref[slot_idx * ROW_PAD:slot_idx * ROW_PAD + n_dev, :].astype(out_ref.dtype)
    first_slot = meta_ref[n_dev + row_base + pl.program_id(0)]
    for step_idx in range(fresh_ref.shape[0]):
        out_ref[0, first_slot + step_idx] = fresh_ref[step_idx, 0]


def merge_heads(own, blocks, fresh_rows, meta, partial_out, row_base, num_rows):
    n_dev = len(blocks) + 1
    chunk_rows, num_slots, head_dim = blocks[0].shape
    n_steps = fresh_rows.shape[0]
    grid_spec = pltpu.PrefetchScalarGridSpec(
        num_scalar_prefetch=1,
        grid=(chunk_rows,),
        in_specs=[pl.BlockSpec((1, num_slots, head_dim), lambda b, meta: (meta[0] * num_rows + row_base + b, 0, 0))]
        + [pl.BlockSpec((1, num_slots, head_dim), lambda b, meta: (b, 0, 0))] * (n_dev - 1)
        + [pl.BlockSpec((n_steps, 1, n_dev, head_dim), lambda b, meta: (0, row_base + b, 0, 0))]
        + ([] if partial_out is None else [pl.BlockSpec(memory_space=pl.ANY)]),
        out_specs=pl.BlockSpec((1, num_slots, n_dev, head_dim), lambda b, meta: (row_base + b, 0, 0, 0)),
        scratch_shapes=[pltpu.VMEM((num_slots * ROW_PAD, head_dim), jnp.float32)],
    )
    return pl.pallas_call(
        functools.partial(merge_kernel, row_base),
        out_shape=jax.ShapeDtypeStruct((num_rows, num_slots, n_dev, head_dim), own.dtype),
        grid_spec=grid_spec,
        input_output_aliases={} if partial_out is None else {n_dev + 2: 0},
        cost_estimate=pl.CostEstimate(flops=10**8, bytes_accessed=4 * n_dev * blocks[0].size, transcendentals=0),
    )(meta, own, *blocks, fresh_rows, *(() if partial_out is None else (partial_out,)))


def solution(mesh):
    n_dev = mesh.shape['x']
    row_spec = P(None, ('dp', 'x'), None)
    cache_in = P('dp', None, 'x', None)
    cache_out = P(('dp', 'x'), None, None, None)

    def local_run(start_pos, hidden_in, k_heads, v_heads, attn_norm, w_q, w_k, w_v, q_norm, k_norm, w_o, mlp_norm, w_gate, w_up, w_down):
        n_steps, num_rows, _ = hidden_in.shape
        all_rows, _, _, head_dim = k_heads.shape
        me = lax.axis_index('x')
        my_pos = lax.dynamic_slice_in_dim(start_pos, me * num_rows, num_rows)
        k_own, v_own = k_heads[:, :, 0], v_heads[:, :, 0]

        def swap(arr, rel_idx):
            return lax.ppermute(arr, 'x', [(d, d ^ rel_idx) for d in range(n_dev)])

        def swap_cache(own, row_base, chunk_rows):
            return [swap(lax.dynamic_slice_in_dim(own, jnp.bitwise_xor(me, rel_idx) * num_rows + row_base, chunk_rows), rel_idx) for rel_idx in SWAP_ORDER]

        cuts_k, cuts_v = cuts(num_rows, K_CUTS), cuts(num_rows, V_CUTS)
        k_got = [swap_cache(k_own, *c) for c in cuts_k]
        positions = my_pos[None, :] + jnp.arange(n_steps)[:, None]
        queries, keys_new, values_new = project(hidden_in, positions, attn_norm, w_q, w_k, w_v, q_norm, k_norm)
        group = queries.shape[2] // n_dev
        q_send = queries.reshape(n_steps, num_rows, n_dev, group, head_dim).transpose(2, 0, 3, 1, 4).reshape(n_dev, n_steps * group, num_rows, head_dim)
        k_send = keys_new.transpose(2, 0, 1, 3)
        v_send = values_new.transpose(2, 0, 1, 3)
        sent = jnp.concatenate([q_send, k_send, v_send], axis=1)
        got = jnp.zeros((n_steps * (group + 2), n_dev, num_rows, head_dim), sent.dtype)
        for rel_idx in range(n_dev):
            peer = jnp.bitwise_xor(me, rel_idx)
            part = lax.dynamic_index_in_dim(sent, peer, 0, keepdims=False)
            part = swap(part, rel_idx) if rel_idx else part
            got = lax.dynamic_update_slice_in_dim(got, part[:, None], peer, 1)
        got = got.reshape(n_steps * (group + 2), all_rows, head_dim)
        q_got = got[:n_steps * group].reshape(n_steps, group, all_rows, head_dim).transpose(0, 2, 1, 3)
        kn_got = got[n_steps * group:n_steps * (group + 1), :, None]
        vn_got = got[n_steps * (group + 1):, :, None]
        mixed = attend(q_got, k_heads, v_heads, kn_got, vn_got, start_pos)
        mixed = mixed.reshape(n_steps, n_dev, num_rows, group, head_dim).transpose(1, 0, 3, 2, 4)
        v_got = [swap_cache(v_own, *c) for c in cuts_v]
        back = jnp.zeros_like(mixed)
        for rel_idx in range(n_dev):
            peer = jnp.bitwise_xor(me, rel_idx)
            part = lax.dynamic_index_in_dim(mixed, peer, 0)
            part = swap(part, rel_idx) if rel_idx else part
            back = lax.dynamic_update_slice_in_dim(back, part, peer, 0)
        attended = back.transpose(1, 3, 0, 2, 4).reshape(n_steps, num_rows, n_dev * group, head_dim)
        out_hidden = finish(hidden_in, attended, w_o, mlp_norm, w_gate, w_up, w_down)
        meta = jnp.concatenate([jnp.bitwise_xor(me, jnp.array((0,) + SWAP_ORDER)), my_pos]).astype(jnp.int32)
        k_out = v_out = None
        for (row_base, chunk_rows), k_blocks in zip(cuts_k, k_got):
            k_out = merge_heads(k_own, k_blocks, keys_new, meta, k_out, row_base, num_rows)
        for (row_base, chunk_rows), v_blocks in zip(cuts_v, v_got):
            v_out = merge_heads(v_own, v_blocks, values_new, meta, v_out, row_base, num_rows)
        return out_hidden, k_out, v_out

    return jax.shard_map(local_run, mesh=mesh, in_specs=(P('dp'), row_spec, cache_in, cache_in) + (P(),) * 11, out_specs=(row_spec, cache_out, cache_out), check_vma=False)
```

```python
import functools
import math

import jax
import jax.numpy as jnp
from jax import lax
from jax.experimental import pallas as pl
from jax.experimental.pallas import tpu as pltpu
from jax.sharding import PartitionSpec as P

EPS = 1e-6
THETA = 1000000.0


def rms_norm(values, gain_vec):
    values32 = values.astype(jnp.float32)
    inv_rms = lax.rsqrt(jnp.mean(values32 * values32, axis=-1, keepdims=True) + EPS)
    return values32 * inv_rms * gain_vec.astype(jnp.float32)


def rotary(values, positions):
    head_dim = values.shape[-1]
    half_dim = head_dim // 2
    inv_freq = jnp.power(THETA, -jnp.arange(half_dim, dtype=jnp.float32) * 2.0 / head_dim)
    angles = positions.astype(jnp.float32)[..., None, None] * inv_freq
    cos_part = jnp.cos(angles)
    sin_part = jnp.sin(angles)
    first_half = values[..., :half_dim]
    second_half = values[..., half_dim:]
    return jnp.concatenate([first_half * cos_part - second_half * sin_part, second_half * cos_part + first_half * sin_part], axis=-1)


def project(hidden, positions, attn_norm, w_q, w_k, w_v, q_norm, k_norm):
    n_steps, num_rows = hidden.shape[0], hidden.shape[1]
    head_dim = q_norm.shape[0]
    normed = rms_norm(hidden, attn_norm).astype(jnp.bfloat16)
    queries = jnp.einsum('sbd,de->sbe', normed, w_q, preferred_element_type=jnp.float32).reshape(n_steps, num_rows, -1, head_dim)
    keys_new = jnp.einsum('sbd,de->sbe', normed, w_k, preferred_element_type=jnp.float32).reshape(n_steps, num_rows, -1, head_dim)
    values_new = jnp.einsum('sbd,de->sbe', normed, w_v, preferred_element_type=jnp.float32).reshape(n_steps, num_rows, -1, head_dim)
    queries = rotary(rms_norm(queries, q_norm), positions).astype(jnp.bfloat16)
    keys_new = rotary(rms_norm(keys_new, k_norm), positions).astype(jnp.bfloat16)
    return queries, keys_new, values_new.astype(jnp.bfloat16)


def attend(queries, cache_k, cache_v, keys_new, values_new, start_pos):
    n_steps, num_rows, n_heads, head_dim = queries.shape
    num_slots, kv_local = cache_k.shape[1], cache_k.shape[2]
    grouped = queries.reshape(n_steps, num_rows, kv_local, n_heads // kv_local, head_dim)
    score_scale = head_dim ** -0.5
    old_scores = jnp.einsum('sbkgd,btkd->bkgst', grouped, cache_k, preferred_element_type=jnp.float32) * score_scale
    old_valid = (jnp.arange(num_slots)[None, :] < start_pos[:, None])[:, None, None, None, :]
    old_scores = jnp.where(old_valid, old_scores, -jnp.inf)
    new_scores = jnp.einsum('sbkgd,jbkd->bkgsj', grouped, keys_new, preferred_element_type=jnp.float32) * score_scale
    new_valid = jnp.arange(n_steps)[:, None] >= jnp.arange(n_steps)[None, :]
    new_scores = jnp.where(new_valid, new_scores, -jnp.inf)
    peak_score = jnp.maximum(jnp.max(old_scores, axis=-1, keepdims=True), jnp.max(new_scores, axis=-1, keepdims=True))
    old_weights = jnp.exp(old_scores - peak_score)
    new_weights = jnp.exp(new_scores - peak_score)
    weight_sum = jnp.sum(old_weights, axis=-1) + jnp.sum(new_weights, axis=-1)
    mixed_vals = jnp.einsum('bkgst,btkd->sbkgd', old_weights.astype(jnp.bfloat16), cache_v, preferred_element_type=jnp.float32)
    mixed_vals = mixed_vals + jnp.einsum('bkgsj,jbkd->sbkgd', new_weights.astype(jnp.bfloat16), values_new, preferred_element_type=jnp.float32)
    mixed_vals = mixed_vals / jnp.transpose(weight_sum, (3, 0, 1, 2))[..., None]
    return mixed_vals.astype(jnp.bfloat16).reshape(n_steps, num_rows, n_heads, head_dim)


def finish(hidden, attended, w_o, mlp_norm, w_gate, w_up, w_down):
    n_steps, num_rows = attended.shape[0], attended.shape[1]
    flat_attn = attended.reshape(n_steps, num_rows, -1)
    attn_out = jnp.einsum('sbe,ed->sbd', flat_attn, w_o, preferred_element_type=jnp.float32)
    residual = (hidden.astype(jnp.float32) + attn_out).astype(jnp.bfloat16)
    normed = rms_norm(residual, mlp_norm).astype(jnp.bfloat16)
    gate_val = jnp.einsum('sbd,df->sbf', normed, w_gate, preferred_element_type=jnp.float32)
    up_val = jnp.einsum('sbd,df->sbf', normed, w_up, preferred_element_type=jnp.float32)
    activated = (jax.nn.silu(gate_val) * up_val).astype(jnp.bfloat16)
    down_val = jnp.einsum('sbf,fd->sbd', activated, w_down, preferred_element_type=jnp.float32)
    return (residual.astype(jnp.float32) + down_val).astype(jnp.bfloat16)


ROW_PAD = 9
MERGE_ROWS = 4
K_CUTS = (8, 20, 32)
SWAP_ORDER = (2, 4, 3, 5, 6, 7, 1)


def cuts(num_rows, ends):
    ends = [num_rows * e // 32 for e in ends]
    return [(lo, hi - lo) for lo, hi in zip([0] + ends[:-1], ends)]


def merge_row(row_idx, block_refs, head_ids, fresh_ref, first_slot, out_ref, wide_ref):
    num_slots, n_dev = out_ref.shape[1], len(block_refs)
    for block_ref, head_idx in zip(block_refs, head_ids):
        wide_ref[pl.ds(head_idx, num_slots, stride=ROW_PAD), :] = block_ref[row_idx].astype(jnp.float32)
    for slot_idx in range(num_slots):
        out_ref[row_idx, slot_idx] = wide_ref[slot_idx * ROW_PAD:slot_idx * ROW_PAD + n_dev, :].astype(out_ref.dtype)
    for step_idx in range(fresh_ref.shape[0]):
        out_ref[row_idx, first_slot + step_idx] = fresh_ref[step_idx, row_idx]


def merge_chunk_kernel(row_base, n_dev, meta_ref, *refs):
    block_refs, fresh_ref, out_ref, wide_ref = refs[:n_dev], refs[n_dev], refs[-2], refs[-1]
    step_rows = out_ref.shape[0]
    head_ids = [meta_ref[rel_idx] for rel_idx in range(n_dev)]

    @pl.loop(0, step_rows)
    def _(row_idx):
        first_slot = meta_ref[n_dev + row_base + pl.program_id(0) * step_rows + row_idx]
        merge_row(row_idx, block_refs, head_ids, fresh_ref, first_slot, out_ref, wide_ref)


def merge_chunk(own, blocks, fresh_rows, meta, partial_out, row_base, num_rows):
    n_dev = len(blocks) + 1
    chunk_rows, num_slots, head_dim = blocks[0].shape
    n_steps = fresh_rows.shape[0]
    step_rows = math.gcd(math.gcd(chunk_rows, row_base), MERGE_ROWS)
    base = row_base // step_rows
    grid_spec = pltpu.PrefetchScalarGridSpec(
        num_scalar_prefetch=1,
        grid=(chunk_rows // step_rows,),
        in_specs=[pl.BlockSpec((step_rows, num_slots, head_dim), lambda b, meta: (meta[0] * (num_rows // step_rows) + base + b, 0, 0))]
        + [pl.BlockSpec((step_rows, num_slots, head_dim), lambda b, meta: (b, 0, 0))] * (n_dev - 1)
        + [pl.BlockSpec((n_steps, step_rows, n_dev, head_dim), lambda b, meta: (0, base + b, 0, 0))]
        + ([] if partial_out is None else [pl.BlockSpec(memory_space=pl.ANY)]),
        out_specs=pl.BlockSpec((step_rows, num_slots, n_dev, head_dim), lambda b, meta: (base + b, 0, 0, 0)),
        scratch_shapes=[pltpu.VMEM((num_slots * ROW_PAD, head_dim), jnp.float32)],
    )
    return pl.pallas_call(
        functools.partial(merge_chunk_kernel, row_base, n_dev),
        out_shape=jax.ShapeDtypeStruct((num_rows, num_slots, n_dev, head_dim), own.dtype),
        grid_spec=grid_spec,
        input_output_aliases={} if partial_out is None else {n_dev + 2: 0},
        cost_estimate=pl.CostEstimate(flops=10**8, bytes_accessed=4 * n_dev * blocks[0].size, transcendentals=0),
    )(meta, own, *blocks, fresh_rows, *(() if partial_out is None else (partial_out,)))


def merge_all_kernel(n_dev, meta_ref, blocks_ref, fresh_ref, out_ref, wide_ref):
    step_rows = out_ref.shape[0]

    @pl.loop(0, step_rows)
    def _(row_idx):
        first_slot = meta_ref[n_dev + pl.program_id(0) * step_rows + row_idx]
        merge_row(row_idx, [blocks_ref.at[h] for h in range(n_dev)], range(n_dev), fresh_ref, first_slot, out_ref, wide_ref)


def merge_all(blocks, fresh_rows, meta):
    n_dev, num_rows, num_slots, head_dim = blocks.shape
    n_steps = fresh_rows.shape[0]
    step_rows = math.gcd(num_rows, MERGE_ROWS)
    return pl.pallas_call(
        functools.partial(merge_all_kernel, n_dev),
        out_shape=jax.ShapeDtypeStruct((num_rows, num_slots, n_dev, head_dim), blocks.dtype),
        grid_spec=pltpu.PrefetchScalarGridSpec(
            num_scalar_prefetch=1,
            grid=(num_rows // step_rows,),
            in_specs=[
                pl.BlockSpec((n_dev, step_rows, num_slots, head_dim), lambda b, meta: (0, b, 0, 0)),
                pl.BlockSpec((n_steps, step_rows, n_dev, head_dim), lambda b, meta: (0, b, 0, 0)),
            ],
            out_specs=pl.BlockSpec((step_rows, num_slots, n_dev, head_dim), lambda b, meta: (b, 0, 0, 0)),
            scratch_shapes=[pltpu.VMEM((num_slots * ROW_PAD, head_dim), jnp.float32)],
        ),
        cost_estimate=pl.CostEstimate(flops=10**8, bytes_accessed=4 * blocks.size, transcendentals=0),
    )(meta, blocks, fresh_rows)


def solution(mesh):
    n_dev = mesh.shape['x']
    row_spec = P(None, ('dp', 'x'), None)
    cache_in = P('dp', None, 'x', None)
    cache_out = P(('dp', 'x'), None, None, None)

    def local_run(start_pos, hidden_in, k_heads, v_heads, attn_norm, w_q, w_k, w_v, q_norm, k_norm, w_o, mlp_norm, w_gate, w_up, w_down):
        n_steps, num_rows, _ = hidden_in.shape
        all_rows, num_slots, _, head_dim = k_heads.shape
        me = lax.axis_index('x')
        my_pos = lax.dynamic_slice_in_dim(start_pos, me * num_rows, num_rows)
        k_own, v_own = k_heads[:, :, 0], v_heads[:, :, 0]

        def swap(arr, rel_idx):
            return lax.ppermute(arr, 'x', [(d, d ^ rel_idx) for d in range(n_dev)])

        def swap_cache(own, row_base, chunk_rows):
            return [swap(lax.dynamic_slice_in_dim(own, jnp.bitwise_xor(me, rel_idx) * num_rows + row_base, chunk_rows), rel_idx) for rel_idx in SWAP_ORDER]

        cuts_k = cuts(num_rows, K_CUTS)
        k_got = [swap_cache(k_own, *c) for c in cuts_k]
        positions = my_pos[None, :] + jnp.arange(n_steps)[:, None]
        queries, keys_new, values_new = project(hidden_in, positions, attn_norm, w_q, w_k, w_v, q_norm, k_norm)
        group = queries.shape[2] // n_dev
        q_send = queries.reshape(n_steps, num_rows, n_dev, group, head_dim).transpose(2, 0, 3, 1, 4).reshape(n_dev, n_steps * group, num_rows, head_dim)
        k_send = keys_new.transpose(2, 0, 1, 3)
        v_send = values_new.transpose(2, 0, 1, 3)
        sent = jnp.concatenate([q_send, k_send, v_send], axis=1)
        got = jnp.zeros((n_steps * (group + 2), n_dev, num_rows, head_dim), sent.dtype)
        for rel_idx in range(n_dev):
            peer = jnp.bitwise_xor(me, rel_idx)
            part = lax.dynamic_index_in_dim(sent, peer, 0, keepdims=False)
            part = swap(part, rel_idx) if rel_idx else part
            got = lax.dynamic_update_slice_in_dim(got, part[:, None], peer, 1)
        got = got.reshape(n_steps * (group + 2), all_rows, head_dim)
        q_got = got[:n_steps * group].reshape(n_steps, group, all_rows, head_dim).transpose(0, 2, 1, 3)
        kn_got = got[n_steps * group:n_steps * (group + 1), :, None]
        vn_got = got[n_steps * (group + 1):, :, None]
        mixed = attend(q_got, k_heads, v_heads, kn_got, vn_got, start_pos)
        mixed = mixed.reshape(n_steps, n_dev, num_rows, group, head_dim).transpose(1, 0, 3, 2, 4)
        v_got = lax.all_to_all(v_own, 'x', 0, 0, tiled=True).reshape(n_dev, num_rows, num_slots, head_dim)
        back = jnp.zeros_like(mixed)
        for rel_idx in range(n_dev):
            peer = jnp.bitwise_xor(me, rel_idx)
            part = lax.dynamic_index_in_dim(mixed, peer, 0)
            part = swap(part, rel_idx) if rel_idx else part
            back = lax.dynamic_update_slice_in_dim(back, part, peer, 0)
        attended = back.transpose(1, 3, 0, 2, 4).reshape(n_steps, num_rows, n_dev * group, head_dim)
        out_hidden = finish(hidden_in, attended, w_o, mlp_norm, w_gate, w_up, w_down)
        meta = jnp.concatenate([jnp.bitwise_xor(me, jnp.array((0,) + SWAP_ORDER)), my_pos]).astype(jnp.int32)
        k_out, v_out = None, merge_all(v_got, values_new, meta)
        for chunk_idx, ((row_base, chunk_rows), k_blocks) in enumerate(zip(cuts_k, k_got)):
            if chunk_idx == len(cuts_k) - 1:
                meta, v_out = lax.optimization_barrier((meta, v_out))
            k_out = merge_chunk(k_own, k_blocks, keys_new, meta, k_out, row_base, num_rows)
        return out_hidden, k_out, v_out

    return jax.shard_map(local_run, mesh=mesh, in_specs=(P('dp'), row_spec, cache_in, cache_in) + (P(),) * 11, out_specs=(row_spec, cache_out, cache_out), check_vma=False)
```

```python
import functools
import math

import jax
import jax.numpy as jnp
from jax import lax
from jax.experimental import pallas as pl
from jax.experimental.pallas import tpu as pltpu
from jax.sharding import PartitionSpec as P

EPS = 1e-6
THETA = 1000000.0


def rms_norm(values, gain_vec):
    values32 = values.astype(jnp.float32)
    inv_rms = lax.rsqrt(jnp.mean(values32 * values32, axis=-1, keepdims=True) + EPS)
    return values32 * inv_rms * gain_vec.astype(jnp.float32)


def rotary(values, positions):
    head_dim = values.shape[-1]
    half_dim = head_dim // 2
    inv_freq = jnp.power(THETA, -jnp.arange(half_dim, dtype=jnp.float32) * 2.0 / head_dim)
    angles = positions.astype(jnp.float32)[..., None, None] * inv_freq
    cos_part = jnp.cos(angles)
    sin_part = jnp.sin(angles)
    first_half = values[..., :half_dim]
    second_half = values[..., half_dim:]
    return jnp.concatenate([first_half * cos_part - second_half * sin_part, second_half * cos_part + first_half * sin_part], axis=-1)


def project(hidden, positions, attn_norm, w_q, w_k, w_v, q_norm, k_norm):
    n_steps, num_rows = hidden.shape[0], hidden.shape[1]
    head_dim = q_norm.shape[0]
    normed = rms_norm(hidden, attn_norm).astype(jnp.bfloat16)
    queries = jnp.einsum('sbd,de->sbe', normed, w_q, preferred_element_type=jnp.float32).reshape(n_steps, num_rows, -1, head_dim)
    keys_new = jnp.einsum('sbd,de->sbe', normed, w_k, preferred_element_type=jnp.float32).reshape(n_steps, num_rows, -1, head_dim)
    values_new = jnp.einsum('sbd,de->sbe', normed, w_v, preferred_element_type=jnp.float32).reshape(n_steps, num_rows, -1, head_dim)
    queries = rotary(rms_norm(queries, q_norm), positions).astype(jnp.bfloat16)
    keys_new = rotary(rms_norm(keys_new, k_norm), positions).astype(jnp.bfloat16)
    return queries, keys_new, values_new.astype(jnp.bfloat16)


def finish(hidden, attended, w_o, mlp_norm, w_gate, w_up, w_down):
    n_steps, num_rows = attended.shape[0], attended.shape[1]
    flat_attn = attended.reshape(n_steps, num_rows, -1)
    attn_out = jnp.einsum('sbe,ed->sbd', flat_attn, w_o, preferred_element_type=jnp.float32)
    residual = (hidden.astype(jnp.float32) + attn_out).astype(jnp.bfloat16)
    normed = rms_norm(residual, mlp_norm).astype(jnp.bfloat16)
    gate_val = jnp.einsum('sbd,df->sbf', normed, w_gate, preferred_element_type=jnp.float32)
    up_val = jnp.einsum('sbd,df->sbf', normed, w_up, preferred_element_type=jnp.float32)
    activated = (jax.nn.silu(gate_val) * up_val).astype(jnp.bfloat16)
    down_val = jnp.einsum('sbf,fd->sbd', activated, w_down, preferred_element_type=jnp.float32)
    return (residual.astype(jnp.float32) + down_val).astype(jnp.bfloat16)


ROW_PAD = 9
MERGE_ROWS = 4
K_CUTS = (8, 18, 26, 32)
SWAP_ORDER = (2, 4, 3, 5, 6, 7, 1)


def cuts(num_rows, ends):
    ends = [num_rows * e // 32 for e in ends]
    return [(lo, hi - lo) for lo, hi in zip([0] + ends[:-1], ends)]


def merge_row(row_idx, block_refs, head_ids, fresh_ref, first_slot, out_ref, wide_ref):
    num_slots, n_dev = out_ref.shape[1], len(block_refs)
    for block_ref, head_idx in zip(block_refs, head_ids):
        wide_ref[pl.ds(head_idx, num_slots, stride=ROW_PAD), :] = block_ref[row_idx].astype(jnp.float32)
    for slot_idx in range(num_slots):
        out_ref[row_idx, slot_idx] = wide_ref[slot_idx * ROW_PAD:slot_idx * ROW_PAD + n_dev, :].astype(out_ref.dtype)
    for step_idx in range(fresh_ref.shape[0]):
        out_ref[row_idx, first_slot + step_idx] = fresh_ref[step_idx, row_idx]


def merge_chunk_kernel(row_base, n_dev, meta_ref, *refs):
    block_refs, fresh_ref, out_ref, wide_ref = refs[:n_dev], refs[n_dev], refs[-2], refs[-1]
    step_rows = out_ref.shape[0]
    head_ids = [meta_ref[rel_idx] for rel_idx in range(n_dev)]

    @pl.loop(0, step_rows)
    def _(row_idx):
        first_slot = meta_ref[n_dev + row_base + pl.program_id(0) * step_rows + row_idx]
        merge_row(row_idx, block_refs, head_ids, fresh_ref, first_slot, out_ref, wide_ref)


def merge_chunk(own, blocks, fresh_rows, meta, partial_out, row_base, num_rows):
    n_dev = len(blocks) + 1
    chunk_rows, num_slots, head_dim = blocks[0].shape
    n_steps = fresh_rows.shape[0]
    step_rows = math.gcd(math.gcd(chunk_rows, row_base), MERGE_ROWS)
    base = row_base // step_rows
    grid_spec = pltpu.PrefetchScalarGridSpec(
        num_scalar_prefetch=1,
        grid=(chunk_rows // step_rows,),
        in_specs=[pl.BlockSpec((step_rows, num_slots, head_dim), lambda b, meta: (meta[0] * (num_rows // step_rows) + base + b, 0, 0))]
        + [pl.BlockSpec((step_rows, num_slots, head_dim), lambda b, meta: (b, 0, 0))] * (n_dev - 1)
        + [pl.BlockSpec((n_steps, step_rows, n_dev, head_dim), lambda b, meta: (0, base + b, 0, 0))]
        + ([] if partial_out is None else [pl.BlockSpec(memory_space=pl.ANY)]),
        out_specs=pl.BlockSpec((step_rows, num_slots, n_dev, head_dim), lambda b, meta: (base + b, 0, 0, 0)),
        scratch_shapes=[pltpu.VMEM((num_slots * ROW_PAD, head_dim), jnp.float32)],
    )
    return pl.pallas_call(
        functools.partial(merge_chunk_kernel, row_base, n_dev),
        out_shape=jax.ShapeDtypeStruct((num_rows, num_slots, n_dev, head_dim), own.dtype),
        grid_spec=grid_spec,
        input_output_aliases={} if partial_out is None else {n_dev + 2: 0},
        cost_estimate=pl.CostEstimate(flops=10**8, bytes_accessed=4 * n_dev * blocks[0].size, transcendentals=0),
    )(meta, own, *blocks, fresh_rows, *(() if partial_out is None else (partial_out,)))


def merge_all_kernel(n_dev, meta_ref, blocks_ref, fresh_ref, out_ref, wide_ref):
    step_rows = out_ref.shape[0]

    @pl.loop(0, step_rows)
    def _(row_idx):
        first_slot = meta_ref[n_dev + pl.program_id(0) * step_rows + row_idx]
        merge_row(row_idx, [blocks_ref.at[h] for h in range(n_dev)], range(n_dev), fresh_ref, first_slot, out_ref, wide_ref)


def merge_all(blocks, fresh_rows, meta):
    n_dev, num_rows, num_slots, head_dim = blocks.shape
    n_steps = fresh_rows.shape[0]
    step_rows = math.gcd(num_rows, MERGE_ROWS)
    return pl.pallas_call(
        functools.partial(merge_all_kernel, n_dev),
        out_shape=jax.ShapeDtypeStruct((num_rows, num_slots, n_dev, head_dim), blocks.dtype),
        grid_spec=pltpu.PrefetchScalarGridSpec(
            num_scalar_prefetch=1,
            grid=(num_rows // step_rows,),
            in_specs=[
                pl.BlockSpec((n_dev, step_rows, num_slots, head_dim), lambda b, meta: (0, b, 0, 0)),
                pl.BlockSpec((n_steps, step_rows, n_dev, head_dim), lambda b, meta: (0, b, 0, 0)),
            ],
            out_specs=pl.BlockSpec((step_rows, num_slots, n_dev, head_dim), lambda b, meta: (b, 0, 0, 0)),
            scratch_shapes=[pltpu.VMEM((num_slots * ROW_PAD, head_dim), jnp.float32)],
        ),
        cost_estimate=pl.CostEstimate(flops=10**8, bytes_accessed=4 * blocks.size, transcendentals=0),
    )(meta, blocks, fresh_rows)


def attend_kernel(n_steps, score_scale, pos_ref, sent_ref, k_ref, v_ref, out_ref, rows_ref, mixed_ref):
    num_sent, step_rows, head_dim = sent_ref.shape[1:]
    num_q = out_ref.shape[1]
    pad_q = num_sent + n_steps
    stride = num_sent + 1 - num_sent % 2
    group = num_q // n_steps
    num_slots = k_ref.shape[1]
    rows_ref[step_rows * stride:, :] = jnp.zeros((rows_ref.shape[0] - step_rows * stride, head_dim), jnp.float32)
    for sent_idx in range(num_sent):
        rows_ref[pl.ds(sent_idx, step_rows, stride=stride), :] = sent_ref[0, sent_idx].astype(jnp.float32)
    rows_ref[pl.ds(num_sent, step_rows, stride=stride), :] = jnp.zeros((step_rows, head_dim), jnp.float32)
    row_step = lax.broadcasted_iota(jnp.int32, (pad_q, pad_q), 0) // group
    col_step = lax.broadcasted_iota(jnp.int32, (pad_q, pad_q), 1) - num_q
    new_valid = (col_step >= 0) & (col_step < n_steps) & (col_step <= row_step)
    slot_ids = lax.broadcasted_iota(jnp.int32, (pad_q, num_slots), 1)
    over_lanes = (((1,), (1,)), ((), ()))
    base = (pl.program_id(0) * pl.num_programs(1) + pl.program_id(1)) * step_rows
    for row_idx in range(step_rows):
        at = row_idx * stride
        queries = rows_ref[at:at + pad_q, :].astype(jnp.bfloat16)
        values_new = rows_ref[at + n_steps:at + n_steps + pad_q, :].astype(jnp.bfloat16)
        old_scores = lax.dot_general(queries, k_ref[row_idx], over_lanes, preferred_element_type=jnp.float32) * score_scale
        new_scores = lax.dot_general(queries, queries, over_lanes, preferred_element_type=jnp.float32) * score_scale
        old_scores = jnp.where(slot_ids < pos_ref[base + row_idx], old_scores, -jnp.inf)
        new_scores = jnp.where(new_valid, new_scores, -jnp.inf)
        peak = jnp.maximum(jnp.max(old_scores, axis=-1, keepdims=True), jnp.max(new_scores, axis=-1, keepdims=True))
        old_weights = jnp.exp(old_scores - peak)
        new_weights = jnp.exp(new_scores - peak)
        weight_sum = jnp.sum(old_weights, axis=-1, keepdims=True) + jnp.sum(new_weights, axis=-1, keepdims=True)
        mixed = jnp.dot(old_weights.astype(jnp.bfloat16), v_ref[row_idx], preferred_element_type=jnp.float32)
        mixed = mixed + jnp.dot(new_weights.astype(jnp.bfloat16), values_new, preferred_element_type=jnp.float32)
        mixed = mixed / weight_sum
        mixed_ref[pl.ds(row_idx, pad_q, stride=step_rows + 1), :] = mixed
    for q_idx in range(num_q):
        at = q_idx * (step_rows + 1)
        out_ref[0, q_idx] = mixed_ref[at:at + step_rows, :].astype(out_ref.dtype)


def attend_local(got, k_own, v_own, start_pos, n_steps):
    n_dev, num_sent, num_rows, head_dim = got.shape
    num_slots = k_own.shape[1]
    num_q = num_sent - 2 * n_steps
    step_rows = 8
    inner = num_rows // step_rows
    pad_q = num_sent + n_steps
    stride = num_sent + 1 - num_sent % 2
    cache_spec = pl.BlockSpec((step_rows, num_slots, head_dim), lambda p, b, pos: (p * inner + b, 0, 0))
    return pl.pallas_call(
        functools.partial(attend_kernel, n_steps, head_dim ** -0.5),
        out_shape=jax.ShapeDtypeStruct((n_dev, num_q, num_rows, head_dim), got.dtype),
        grid_spec=pltpu.PrefetchScalarGridSpec(
            num_scalar_prefetch=1,
            grid=(n_dev, inner),
            in_specs=[pl.BlockSpec((1, num_sent, step_rows, head_dim), lambda p, b, pos: (p, 0, b, 0)), cache_spec, cache_spec],
            out_specs=pl.BlockSpec((1, num_q, step_rows, head_dim), lambda p, b, pos: (p, 0, b, 0)),
            scratch_shapes=[
                pltpu.VMEM((step_rows * stride + 16, head_dim), jnp.float32),
                pltpu.VMEM((pad_q * (step_rows + 1) + 8, head_dim), jnp.float32),
            ],
        ),
        cost_estimate=pl.CostEstimate(flops=10**9, bytes_accessed=4 * k_own.size, transcendentals=0),
    )(start_pos, got, k_own, v_own)


def solution(mesh):
    n_dev = mesh.shape['x']
    row_spec = P(None, ('dp', 'x'), None)
    cache_in = P('dp', None, 'x', None)
    cache_out = P(('dp', 'x'), None, None, None)

    def local_run(start_pos, hidden_in, k_heads, v_heads, attn_norm, w_q, w_k, w_v, q_norm, k_norm, w_o, mlp_norm, w_gate, w_up, w_down):
        n_steps, num_rows, _ = hidden_in.shape
        _, num_slots, _, head_dim = k_heads.shape
        me = lax.axis_index('x')
        my_pos = lax.dynamic_slice_in_dim(start_pos, me * num_rows, num_rows)
        k_own, v_own = k_heads[:, :, 0], v_heads[:, :, 0]

        def swap(arr, rel_idx):
            return lax.ppermute(arr, 'x', [(d, d ^ rel_idx) for d in range(n_dev)])

        def swap_cache(own, row_base, chunk_rows):
            return [swap(lax.dynamic_slice_in_dim(own, jnp.bitwise_xor(me, rel_idx) * num_rows + row_base, chunk_rows), rel_idx) for rel_idx in SWAP_ORDER]

        cuts_k = cuts(num_rows, K_CUTS)
        k_got = [swap_cache(k_own, *c) for c in cuts_k]
        positions = my_pos[None, :] + jnp.arange(n_steps)[:, None]
        queries, keys_new, values_new = project(hidden_in, positions, attn_norm, w_q, w_k, w_v, q_norm, k_norm)
        group = queries.shape[2] // n_dev
        q_send = queries.reshape(n_steps, num_rows, n_dev, group, head_dim).transpose(2, 0, 3, 1, 4).reshape(n_dev, n_steps * group, num_rows, head_dim)
        k_send = keys_new.transpose(2, 0, 1, 3)
        v_send = values_new.transpose(2, 0, 1, 3)
        sent = jnp.concatenate([q_send, k_send, v_send], axis=1)
        got = lax.all_to_all(sent, 'x', 0, 0, tiled=True)
        mixed = attend_local(got, k_own, v_own, start_pos, n_steps)
        v_got = lax.all_to_all(v_own, 'x', 0, 0, tiled=True).reshape(n_dev, num_rows, num_slots, head_dim)
        back = lax.all_to_all(mixed, 'x', 0, 0, tiled=True)
        attended = back.reshape(n_dev, n_steps, group, num_rows, head_dim).transpose(1, 3, 0, 2, 4).reshape(n_steps, num_rows, n_dev * group, head_dim)
        out_hidden = finish(hidden_in, attended, w_o, mlp_norm, w_gate, w_up, w_down)
        meta = jnp.concatenate([jnp.bitwise_xor(me, jnp.array((0,) + SWAP_ORDER)), my_pos]).astype(jnp.int32)
        k_out, v_out = None, merge_all(v_got, values_new, meta)
        for chunk_idx, ((row_base, chunk_rows), k_blocks) in enumerate(zip(cuts_k, k_got)):
            if chunk_idx == len(cuts_k) - 1:
                meta, v_out = lax.optimization_barrier((meta, v_out))
            k_out = merge_chunk(k_own, k_blocks, keys_new, meta, k_out, row_base, num_rows)
        return out_hidden, k_out, v_out

    return jax.shard_map(local_run, mesh=mesh, in_specs=(P('dp'), row_spec, cache_in, cache_in) + (P(),) * 11, out_specs=(row_spec, cache_out, cache_out), check_vma=False)
```

```python
import functools
import math

import jax
import jax.numpy as jnp
from jax import lax
from jax.experimental import pallas as pl
from jax.experimental.pallas import tpu as pltpu
from jax.sharding import PartitionSpec as P

EPS = 1e-6
THETA = 1000000.0


def rms_norm(values, gain_vec):
    values32 = values.astype(jnp.float32)
    inv_rms = lax.rsqrt(jnp.mean(values32 * values32, axis=-1, keepdims=True) + EPS)
    return values32 * inv_rms * gain_vec.astype(jnp.float32)


def rotary(values, positions):
    head_dim = values.shape[-1]
    half_dim = head_dim // 2
    inv_freq = jnp.power(THETA, -jnp.arange(half_dim, dtype=jnp.float32) * 2.0 / head_dim)
    angles = positions.astype(jnp.float32)[..., None, None] * inv_freq
    cos_part = jnp.cos(angles)
    sin_part = jnp.sin(angles)
    first_half = values[..., :half_dim]
    second_half = values[..., half_dim:]
    return jnp.concatenate([first_half * cos_part - second_half * sin_part, second_half * cos_part + first_half * sin_part], axis=-1)


def project(hidden, positions, attn_norm, w_q, w_k, w_v, q_norm, k_norm):
    n_steps, num_rows = hidden.shape[0], hidden.shape[1]
    head_dim = q_norm.shape[0]
    normed = rms_norm(hidden, attn_norm).astype(jnp.bfloat16)
    queries = jnp.einsum('sbd,de->sbe', normed, w_q, preferred_element_type=jnp.float32).reshape(n_steps, num_rows, -1, head_dim)
    keys_new = jnp.einsum('sbd,de->sbe', normed, w_k, preferred_element_type=jnp.float32).reshape(n_steps, num_rows, -1, head_dim)
    values_new = jnp.einsum('sbd,de->sbe', normed, w_v, preferred_element_type=jnp.float32).reshape(n_steps, num_rows, -1, head_dim)
    queries = rotary(rms_norm(queries, q_norm), positions).astype(jnp.bfloat16)
    keys_new = rotary(rms_norm(keys_new, k_norm), positions).astype(jnp.bfloat16)
    return queries, keys_new, values_new.astype(jnp.bfloat16)


def finish(hidden, attended, w_o, mlp_norm, w_gate, w_up, w_down):
    n_steps, num_rows = attended.shape[0], attended.shape[1]
    flat_attn = attended.reshape(n_steps, num_rows, -1)
    attn_out = jnp.einsum('sbe,ed->sbd', flat_attn, w_o, preferred_element_type=jnp.float32)
    residual = (hidden.astype(jnp.float32) + attn_out).astype(jnp.bfloat16)
    normed = rms_norm(residual, mlp_norm).astype(jnp.bfloat16)
    gate_val = jnp.einsum('sbd,df->sbf', normed, w_gate, preferred_element_type=jnp.float32)
    up_val = jnp.einsum('sbd,df->sbf', normed, w_up, preferred_element_type=jnp.float32)
    activated = (jax.nn.silu(gate_val) * up_val).astype(jnp.bfloat16)
    down_val = jnp.einsum('sbf,fd->sbd', activated, w_down, preferred_element_type=jnp.float32)
    return (residual.astype(jnp.float32) + down_val).astype(jnp.bfloat16)


ROW_PAD = 9
MERGE_ROWS = 4
K_CUTS = (8, 16, 28, 32)
SWAP_ORDER = (2, 4, 3, 5, 6, 7, 1)


def cuts(num_rows, ends):
    ends = [num_rows * e // 32 for e in ends]
    return [(lo, hi - lo) for lo, hi in zip([0] + ends[:-1], ends)]


def merge_row(row_idx, block_refs, head_ids, fresh_ref, first_slot, out_ref, wide_ref):
    num_slots, n_dev = out_ref.shape[1], len(block_refs)
    for block_ref, head_idx in zip(block_refs, head_ids):
        wide_ref[pl.ds(head_idx, num_slots, stride=ROW_PAD), :] = block_ref[row_idx].astype(jnp.float32)
    for slot_idx in range(num_slots):
        out_ref[row_idx, slot_idx] = wide_ref[slot_idx * ROW_PAD:slot_idx * ROW_PAD + n_dev, :].astype(out_ref.dtype)
    for step_idx in range(fresh_ref.shape[0]):
        out_ref[row_idx, first_slot + step_idx] = fresh_ref[step_idx, row_idx]


def merge_chunk_kernel(row_base, n_dev, meta_ref, *refs):
    block_refs, fresh_ref, out_ref, wide_ref = refs[:n_dev], refs[n_dev], refs[-2], refs[-1]
    step_rows = out_ref.shape[0]
    head_ids = [meta_ref[rel_idx] for rel_idx in range(n_dev)]

    @pl.loop(0, step_rows)
    def _(row_idx):
        first_slot = meta_ref[n_dev + row_base + pl.program_id(0) * step_rows + row_idx]
        merge_row(row_idx, block_refs, head_ids, fresh_ref, first_slot, out_ref, wide_ref)


def merge_chunk(own, blocks, fresh_rows, meta, partial_out, row_base, num_rows):
    n_dev = len(blocks) + 1
    chunk_rows, num_slots, head_dim = blocks[0].shape
    n_steps = fresh_rows.shape[0]
    step_rows = math.gcd(math.gcd(chunk_rows, row_base), MERGE_ROWS)
    base = row_base // step_rows
    grid_spec = pltpu.PrefetchScalarGridSpec(
        num_scalar_prefetch=1,
        grid=(chunk_rows // step_rows,),
        in_specs=[pl.BlockSpec((step_rows, num_slots, head_dim), lambda b, meta: (meta[0] * (num_rows // step_rows) + base + b, 0, 0))]
        + [pl.BlockSpec((step_rows, num_slots, head_dim), lambda b, meta: (b, 0, 0))] * (n_dev - 1)
        + [pl.BlockSpec((n_steps, step_rows, n_dev, head_dim), lambda b, meta: (0, base + b, 0, 0))]
        + ([] if partial_out is None else [pl.BlockSpec(memory_space=pl.ANY)]),
        out_specs=pl.BlockSpec((step_rows, num_slots, n_dev, head_dim), lambda b, meta: (base + b, 0, 0, 0)),
        scratch_shapes=[pltpu.VMEM((num_slots * ROW_PAD, head_dim), jnp.float32)],
    )
    return pl.pallas_call(
        functools.partial(merge_chunk_kernel, row_base, n_dev),
        out_shape=jax.ShapeDtypeStruct((num_rows, num_slots, n_dev, head_dim), own.dtype),
        grid_spec=grid_spec,
        input_output_aliases={} if partial_out is None else {n_dev + 2: 0},
        cost_estimate=pl.CostEstimate(flops=10**8, bytes_accessed=4 * n_dev * blocks[0].size, transcendentals=0),
    )(meta, own, *blocks, fresh_rows, *(() if partial_out is None else (partial_out,)))


def merge_all_kernel(n_dev, meta_ref, blocks_ref, fresh_ref, out_ref, wide_ref):
    step_rows = out_ref.shape[0]

    @pl.loop(0, step_rows)
    def _(row_idx):
        first_slot = meta_ref[n_dev + pl.program_id(0) * step_rows + row_idx]
        merge_row(row_idx, [blocks_ref.at[h] for h in range(n_dev)], range(n_dev), fresh_ref, first_slot, out_ref, wide_ref)


def merge_all(blocks, fresh_rows, meta):
    n_dev, num_rows, num_slots, head_dim = blocks.shape
    n_steps = fresh_rows.shape[0]
    step_rows = math.gcd(num_rows, 2 * MERGE_ROWS)
    return pl.pallas_call(
        functools.partial(merge_all_kernel, n_dev),
        out_shape=jax.ShapeDtypeStruct((num_rows, num_slots, n_dev, head_dim), blocks.dtype),
        grid_spec=pltpu.PrefetchScalarGridSpec(
            num_scalar_prefetch=1,
            grid=(num_rows // step_rows,),
            in_specs=[
                pl.BlockSpec((n_dev, step_rows, num_slots, head_dim), lambda b, meta: (0, b, 0, 0)),
                pl.BlockSpec((n_steps, step_rows, n_dev, head_dim), lambda b, meta: (0, b, 0, 0)),
            ],
            out_specs=pl.BlockSpec((step_rows, num_slots, n_dev, head_dim), lambda b, meta: (b, 0, 0, 0)),
            scratch_shapes=[pltpu.VMEM((num_slots * ROW_PAD, head_dim), jnp.float32)],
        ),
        cost_estimate=pl.CostEstimate(flops=10**8, bytes_accessed=4 * blocks.size, transcendentals=0),
    )(meta, blocks, fresh_rows)


def attend_kernel(n_steps, score_scale, pos_ref, sent_ref, k_ref, v_ref, out_ref, rows_ref, mixed_ref):
    num_sent, step_rows, head_dim = sent_ref.shape[1:]
    num_q = out_ref.shape[1]
    pad_q = num_sent + n_steps
    stride = num_sent + 1 - num_sent % 2
    group = num_q // n_steps
    num_slots = k_ref.shape[1]
    rows_ref[step_rows * stride:, :] = jnp.zeros((rows_ref.shape[0] - step_rows * stride, head_dim), jnp.float32)
    for sent_idx in range(num_sent):
        rows_ref[pl.ds(sent_idx, step_rows, stride=stride), :] = sent_ref[0, sent_idx].astype(jnp.float32)
    rows_ref[pl.ds(num_sent, step_rows, stride=stride), :] = jnp.zeros((step_rows, head_dim), jnp.float32)
    row_step = lax.broadcasted_iota(jnp.int32, (pad_q, pad_q), 0) // group
    col_step = lax.broadcasted_iota(jnp.int32, (pad_q, pad_q), 1) - num_q
    new_valid = (col_step >= 0) & (col_step < n_steps) & (col_step <= row_step)
    slot_ids = lax.broadcasted_iota(jnp.int32, (pad_q, num_slots), 1)
    over_lanes = (((1,), (1,)), ((), ()))
    base = (pl.program_id(0) * pl.num_programs(1) + pl.program_id(1)) * step_rows
    for row_idx in range(step_rows):
        at = row_idx * stride
        queries = rows_ref[at:at + pad_q, :].astype(jnp.bfloat16)
        values_new = rows_ref[at + n_steps:at + n_steps + pad_q, :].astype(jnp.bfloat16)
        old_scores = lax.dot_general(queries, k_ref[row_idx], over_lanes, preferred_element_type=jnp.float32) * score_scale
        new_scores = lax.dot_general(queries, queries, over_lanes, preferred_element_type=jnp.float32) * score_scale
        old_scores = jnp.where(slot_ids < pos_ref[base + row_idx], old_scores, -jnp.inf)
        new_scores = jnp.where(new_valid, new_scores, -jnp.inf)
        peak = jnp.maximum(jnp.max(old_scores, axis=-1, keepdims=True), jnp.max(new_scores, axis=-1, keepdims=True))
        old_weights = jnp.exp(old_scores - peak)
        new_weights = jnp.exp(new_scores - peak)
        weight_sum = jnp.sum(old_weights, axis=-1, keepdims=True) + jnp.sum(new_weights, axis=-1, keepdims=True)
        mixed = jnp.dot(old_weights.astype(jnp.bfloat16), v_ref[row_idx], preferred_element_type=jnp.float32)
        mixed = mixed + jnp.dot(new_weights.astype(jnp.bfloat16), values_new, preferred_element_type=jnp.float32)
        mixed = mixed / weight_sum
        mixed_ref[pl.ds(row_idx, pad_q, stride=step_rows + 1), :] = mixed
    for q_idx in range(num_q):
        at = q_idx * (step_rows + 1)
        out_ref[0, q_idx] = mixed_ref[at:at + step_rows, :].astype(out_ref.dtype)


def attend_local(got, k_own, v_own, start_pos, n_steps):
    n_dev, num_sent, num_rows, head_dim = got.shape
    num_slots = k_own.shape[1]
    num_q = num_sent - 2 * n_steps
    step_rows = num_rows
    inner = num_rows // step_rows
    pad_q = num_sent + n_steps
    stride = num_sent + 1 - num_sent % 2
    cache_spec = pl.BlockSpec((step_rows, num_slots, head_dim), lambda p, b, pos: (p * inner + b, 0, 0))
    return pl.pallas_call(
        functools.partial(attend_kernel, n_steps, head_dim ** -0.5),
        out_shape=jax.ShapeDtypeStruct((n_dev, num_q, num_rows, head_dim), got.dtype),
        grid_spec=pltpu.PrefetchScalarGridSpec(
            num_scalar_prefetch=1,
            grid=(n_dev, inner),
            in_specs=[pl.BlockSpec((1, num_sent, step_rows, head_dim), lambda p, b, pos: (p, 0, b, 0)), cache_spec, cache_spec],
            out_specs=pl.BlockSpec((1, num_q, step_rows, head_dim), lambda p, b, pos: (p, 0, b, 0)),
            scratch_shapes=[
                pltpu.VMEM((step_rows * stride + 16, head_dim), jnp.float32),
                pltpu.VMEM((pad_q * (step_rows + 1) + 8, head_dim), jnp.float32),
            ],
        ),
        cost_estimate=pl.CostEstimate(flops=10**9, bytes_accessed=4 * k_own.size, transcendentals=0),
    )(start_pos, got, k_own, v_own)


def solution(mesh):
    n_dev = mesh.shape['x']
    row_spec = P(None, ('dp', 'x'), None)
    cache_in = P('dp', None, 'x', None)
    cache_out = P(('dp', 'x'), None, None, None)

    def local_run(start_pos, hidden_in, k_heads, v_heads, attn_norm, w_q, w_k, w_v, q_norm, k_norm, w_o, mlp_norm, w_gate, w_up, w_down):
        n_steps, num_rows, _ = hidden_in.shape
        _, num_slots, _, head_dim = k_heads.shape
        me = lax.axis_index('x')
        my_pos = lax.dynamic_slice_in_dim(start_pos, me * num_rows, num_rows)
        k_own, v_own = k_heads[:, :, 0], v_heads[:, :, 0]

        def swap(arr, rel_idx):
            return lax.ppermute(arr, 'x', [(d, d ^ rel_idx) for d in range(n_dev)])

        def swap_cache(own, row_base, chunk_rows):
            return [swap(lax.dynamic_slice_in_dim(own, jnp.bitwise_xor(me, rel_idx) * num_rows + row_base, chunk_rows), rel_idx) for rel_idx in SWAP_ORDER]

        cuts_k = cuts(num_rows, K_CUTS)
        positions = my_pos[None, :] + jnp.arange(n_steps)[:, None]
        queries, keys_new, values_new = project(hidden_in, positions, attn_norm, w_q, w_k, w_v, q_norm, k_norm)
        group = queries.shape[2] // n_dev
        q_send = queries.reshape(n_steps, num_rows, n_dev, group, head_dim).transpose(2, 0, 3, 1, 4).reshape(n_dev, n_steps * group, num_rows, head_dim)
        k_send = keys_new.transpose(2, 0, 1, 3)
        v_send = values_new.transpose(2, 0, 1, 3)
        sent = jnp.concatenate([q_send, k_send, v_send], axis=1)
        k_later, sent = lax.optimization_barrier((k_own, sent))
        k_got = [swap_cache(k_later if i else k_own, *c) for i, c in enumerate(cuts_k)]
        got = lax.all_to_all(sent, 'x', 0, 0, tiled=True)
        mixed = attend_local(got, k_own, v_own, start_pos, n_steps)
        v_got = lax.all_to_all(v_own, 'x', 0, 0, tiled=True).reshape(n_dev, num_rows, num_slots, head_dim)
        back = lax.all_to_all(mixed, 'x', 0, 0, tiled=True)
        attended = back.reshape(n_dev, n_steps, group, num_rows, head_dim).transpose(1, 3, 0, 2, 4).reshape(n_steps, num_rows, n_dev * group, head_dim)
        out_hidden = finish(hidden_in, attended, w_o, mlp_norm, w_gate, w_up, w_down)
        meta = jnp.concatenate([jnp.bitwise_xor(me, jnp.array((0,) + SWAP_ORDER)), my_pos]).astype(jnp.int32)
        k_out, v_out = None, merge_all(v_got, values_new, meta)
        for chunk_idx, ((row_base, chunk_rows), k_blocks) in enumerate(zip(cuts_k, k_got)):
            if chunk_idx == 2:
                meta, out_hidden = lax.optimization_barrier((meta, out_hidden))
            if chunk_idx == len(cuts_k) - 1:
                meta, v_out = lax.optimization_barrier((meta, v_out))
            k_out = merge_chunk(k_own, k_blocks, keys_new, meta, k_out, row_base, num_rows)
        return out_hidden, k_out, v_out

    return jax.shard_map(local_run, mesh=mesh, in_specs=(P('dp'), row_spec, cache_in, cache_in) + (P(),) * 11, out_specs=(row_spec, cache_out, cache_out), check_vma=False)
```

```python
import functools
import math

import jax
import jax.numpy as jnp
from jax import lax
from jax.experimental import pallas as pl
from jax.experimental.pallas import tpu as pltpu
from jax.sharding import PartitionSpec as P

EPS = 1e-6
THETA = 1000000.0


def rms_norm(values, gain_vec):
    values32 = values.astype(jnp.float32)
    inv_rms = lax.rsqrt(jnp.mean(values32 * values32, axis=-1, keepdims=True) + EPS)
    return values32 * inv_rms * gain_vec.astype(jnp.float32)


def rotary(values, positions):
    head_dim = values.shape[-1]
    half_dim = head_dim // 2
    inv_freq = jnp.power(THETA, -jnp.arange(half_dim, dtype=jnp.float32) * 2.0 / head_dim)
    angles = positions.astype(jnp.float32)[..., None, None] * inv_freq
    cos_part = jnp.cos(angles)
    sin_part = jnp.sin(angles)
    first_half = values[..., :half_dim]
    second_half = values[..., half_dim:]
    return jnp.concatenate([first_half * cos_part - second_half * sin_part, second_half * cos_part + first_half * sin_part], axis=-1)


def project(hidden, positions, attn_norm, w_q, w_k, w_v, q_norm, k_norm):
    n_steps, num_rows = hidden.shape[0], hidden.shape[1]
    head_dim = q_norm.shape[0]
    normed = rms_norm(hidden, attn_norm).astype(jnp.bfloat16)
    queries = jnp.einsum('sbd,de->sbe', normed, w_q, preferred_element_type=jnp.float32).reshape(n_steps, num_rows, -1, head_dim)
    keys_new = jnp.einsum('sbd,de->sbe', normed, w_k, preferred_element_type=jnp.float32).reshape(n_steps, num_rows, -1, head_dim)
    values_new = jnp.einsum('sbd,de->sbe', normed, w_v, preferred_element_type=jnp.float32).reshape(n_steps, num_rows, -1, head_dim)
    queries = rotary(rms_norm(queries, q_norm), positions).astype(jnp.bfloat16)
    keys_new = rotary(rms_norm(keys_new, k_norm), positions).astype(jnp.bfloat16)
    return queries, keys_new, values_new.astype(jnp.bfloat16)


def finish(hidden, attended, w_o, mlp_norm, w_gate, w_up, w_down):
    n_steps, num_rows = attended.shape[0], attended.shape[1]
    flat_attn = attended.reshape(n_steps, num_rows, -1)
    attn_out = jnp.einsum('sbe,ed->sbd', flat_attn, w_o, preferred_element_type=jnp.float32)
    residual = (hidden.astype(jnp.float32) + attn_out).astype(jnp.bfloat16)
    normed = rms_norm(residual, mlp_norm).astype(jnp.bfloat16)
    gate_val = jnp.einsum('sbd,df->sbf', normed, w_gate, preferred_element_type=jnp.float32)
    up_val = jnp.einsum('sbd,df->sbf', normed, w_up, preferred_element_type=jnp.float32)
    activated = (jax.nn.silu(gate_val) * up_val).astype(jnp.bfloat16)
    down_val = jnp.einsum('sbf,fd->sbd', activated, w_down, preferred_element_type=jnp.float32)
    return (residual.astype(jnp.float32) + down_val).astype(jnp.bfloat16)


ROW_PAD = 9
MERGE_ROWS = 4
ATTEND_ROWS = 8
K_CUTS = (8, 16, 28, 32)
SWAP_ORDER = (2, 4, 3, 5, 6, 7, 1)


def cuts(num_rows, ends):
    ends = [num_rows * e // 32 for e in ends]
    return [(lo, hi - lo) for lo, hi in zip([0] + ends[:-1], ends)]


def merge_row(row_idx, block_refs, head_ids, fresh_ref, first_slot, out_ref, wide_ref):
    num_slots, n_dev = out_ref.shape[1], len(block_refs)
    for block_ref, head_idx in zip(block_refs, head_ids):
        wide_ref[pl.ds(head_idx, num_slots, stride=ROW_PAD), :] = block_ref[row_idx].astype(jnp.float32)
    for slot_idx in range(num_slots):
        out_ref[row_idx, slot_idx] = wide_ref[slot_idx * ROW_PAD:slot_idx * ROW_PAD + n_dev, :].astype(out_ref.dtype)
    for step_idx in range(fresh_ref.shape[0]):
        out_ref[row_idx, first_slot + step_idx] = fresh_ref[step_idx, row_idx]


def merge_chunk_kernel(row_base, n_dev, meta_ref, *refs):
    block_refs, fresh_ref, out_ref, wide_ref = refs[:n_dev], refs[n_dev], refs[-2], refs[-1]
    step_rows = out_ref.shape[0]
    head_ids = [meta_ref[rel_idx] for rel_idx in range(n_dev)]

    @pl.loop(0, step_rows)
    def _(row_idx):
        first_slot = meta_ref[n_dev + row_base + pl.program_id(0) * step_rows + row_idx]
        merge_row(row_idx, block_refs, head_ids, fresh_ref, first_slot, out_ref, wide_ref)


def merge_chunk(own, blocks, fresh_rows, meta, partial_out, row_base, num_rows):
    n_dev = len(blocks) + 1
    chunk_rows, num_slots, head_dim = blocks[0].shape
    n_steps = fresh_rows.shape[0]
    step_rows = math.gcd(math.gcd(chunk_rows, row_base), MERGE_ROWS)
    base = row_base // step_rows
    grid_spec = pltpu.PrefetchScalarGridSpec(
        num_scalar_prefetch=1,
        grid=(chunk_rows // step_rows,),
        in_specs=[pl.BlockSpec((step_rows, num_slots, head_dim), lambda b, meta: (meta[0] * (num_rows // step_rows) + base + b, 0, 0))]
        + [pl.BlockSpec((step_rows, num_slots, head_dim), lambda b, meta: (b, 0, 0))] * (n_dev - 1)
        + [pl.BlockSpec((n_steps, step_rows, n_dev, head_dim), lambda b, meta: (0, base + b, 0, 0))]
        + ([] if partial_out is None else [pl.BlockSpec(memory_space=pl.ANY)]),
        out_specs=pl.BlockSpec((step_rows, num_slots, n_dev, head_dim), lambda b, meta: (base + b, 0, 0, 0)),
        scratch_shapes=[pltpu.VMEM((num_slots * ROW_PAD, head_dim), jnp.float32)],
    )
    return pl.pallas_call(
        functools.partial(merge_chunk_kernel, row_base, n_dev),
        out_shape=jax.ShapeDtypeStruct((num_rows, num_slots, n_dev, head_dim), own.dtype),
        grid_spec=grid_spec,
        input_output_aliases={} if partial_out is None else {n_dev + 2: 0},
        cost_estimate=pl.CostEstimate(flops=10**8, bytes_accessed=4 * n_dev * blocks[0].size, transcendentals=0),
    )(meta, own, *blocks, fresh_rows, *(() if partial_out is None else (partial_out,)))


def merge_all_kernel(n_dev, meta_ref, blocks_ref, fresh_ref, out_ref, wide_ref):
    step_rows = out_ref.shape[0]

    @pl.loop(0, step_rows)
    def _(row_idx):
        first_slot = meta_ref[n_dev + pl.program_id(0) * step_rows + row_idx]
        merge_row(row_idx, [blocks_ref.at[h] for h in range(n_dev)], range(n_dev), fresh_ref, first_slot, out_ref, wide_ref)


def merge_all(blocks, fresh_rows, meta):
    n_dev, num_rows, num_slots, head_dim = blocks.shape
    n_steps = fresh_rows.shape[0]
    step_rows = math.gcd(num_rows, 2 * MERGE_ROWS)
    return pl.pallas_call(
        functools.partial(merge_all_kernel, n_dev),
        out_shape=jax.ShapeDtypeStruct((num_rows, num_slots, n_dev, head_dim), blocks.dtype),
        grid_spec=pltpu.PrefetchScalarGridSpec(
            num_scalar_prefetch=1,
            grid=(num_rows // step_rows,),
            in_specs=[
                pl.BlockSpec((n_dev, step_rows, num_slots, head_dim), lambda b, meta: (0, b, 0, 0)),
                pl.BlockSpec((n_steps, step_rows, n_dev, head_dim), lambda b, meta: (0, b, 0, 0)),
            ],
            out_specs=pl.BlockSpec((step_rows, num_slots, n_dev, head_dim), lambda b, meta: (b, 0, 0, 0)),
            scratch_shapes=[pltpu.VMEM((num_slots * ROW_PAD, head_dim), jnp.float32)],
        ),
        cost_estimate=pl.CostEstimate(flops=10**8, bytes_accessed=4 * blocks.size, transcendentals=0),
    )(meta, blocks, fresh_rows)


def attend_kernel(n_steps, score_scale, pos_ref, sent_ref, k_ref, v_ref, out_ref, rows_ref, mixed_ref):
    num_sent, step_rows, head_dim = sent_ref.shape[1:]
    num_q = out_ref.shape[1]
    pad_q = num_sent + n_steps
    stride = num_sent + 1 - num_sent % 2
    group = num_q // n_steps
    num_slots = k_ref.shape[1]
    rows_ref[step_rows * stride:, :] = jnp.zeros((rows_ref.shape[0] - step_rows * stride, head_dim), jnp.float32)
    for sent_idx in range(num_sent):
        rows_ref[pl.ds(sent_idx, step_rows, stride=stride), :] = sent_ref[0, sent_idx].astype(jnp.float32)
    rows_ref[pl.ds(num_sent, step_rows, stride=stride), :] = jnp.zeros((step_rows, head_dim), jnp.float32)
    row_step = lax.broadcasted_iota(jnp.int32, (pad_q, pad_q), 0) // group
    col_step = lax.broadcasted_iota(jnp.int32, (pad_q, pad_q), 1) - num_q
    new_valid = (col_step >= 0) & (col_step < n_steps) & (col_step <= row_step)
    slot_ids = lax.broadcasted_iota(jnp.int32, (pad_q, num_slots), 1)
    over_lanes = (((1,), (1,)), ((), ()))
    base = (pl.program_id(0) * pl.num_programs(1) + pl.program_id(1)) * step_rows
    for first_row in range(0, step_rows, ATTEND_ROWS):
        rows = range(first_row, min(first_row + ATTEND_ROWS, step_rows))
        queries = [rows_ref[r * stride:r * stride + pad_q, :].astype(jnp.bfloat16) for r in rows]
        old = [lax.dot_general(q, k_ref[r], over_lanes, preferred_element_type=jnp.float32) for r, q in zip(rows, queries)]
        new = [lax.dot_general(q, q, over_lanes, preferred_element_type=jnp.float32) for q in queries]
        old = [jnp.where(slot_ids < pos_ref[base + r], s * score_scale, -jnp.inf) for r, s in zip(rows, old)]
        new = [jnp.where(new_valid, s * score_scale, -jnp.inf) for s in new]
        peak = [jnp.maximum(jnp.max(a, axis=-1, keepdims=True), jnp.max(c, axis=-1, keepdims=True)) for a, c in zip(old, new)]
        old = [jnp.exp(s - m) for s, m in zip(old, peak)]
        new = [jnp.exp(s - m) for s, m in zip(new, peak)]
        weight_sum = [jnp.sum(a, axis=-1, keepdims=True) + jnp.sum(c, axis=-1, keepdims=True) for a, c in zip(old, new)]
        mixed = [jnp.dot(w.astype(jnp.bfloat16), v_ref[r], preferred_element_type=jnp.float32) for r, w in zip(rows, old)]
        values_new = [rows_ref[r * stride + n_steps:r * stride + n_steps + pad_q, :].astype(jnp.bfloat16) for r in rows]
        fresh = [jnp.dot(w.astype(jnp.bfloat16), v, preferred_element_type=jnp.float32) for w, v in zip(new, values_new)]
        mixed = [(a + c) / s for a, c, s in zip(mixed, fresh, weight_sum)]
        for r, o in zip(rows, mixed):
            mixed_ref[pl.ds(r, pad_q, stride=step_rows + 1), :] = o
    for q_idx in range(num_q):
        at = q_idx * (step_rows + 1)
        out_ref[0, q_idx] = mixed_ref[at:at + step_rows, :].astype(out_ref.dtype)


def attend_local(got, k_own, v_own, start_pos, n_steps):
    n_dev, num_sent, num_rows, head_dim = got.shape
    num_slots = k_own.shape[1]
    num_q = num_sent - 2 * n_steps
    step_rows = num_rows
    inner = num_rows // step_rows
    pad_q = num_sent + n_steps
    stride = num_sent + 1 - num_sent % 2
    cache_spec = pl.BlockSpec((step_rows, num_slots, head_dim), lambda p, b, pos: (p * inner + b, 0, 0))
    return pl.pallas_call(
        functools.partial(attend_kernel, n_steps, head_dim ** -0.5),
        out_shape=jax.ShapeDtypeStruct((n_dev, num_q, num_rows, head_dim), got.dtype),
        grid_spec=pltpu.PrefetchScalarGridSpec(
            num_scalar_prefetch=1,
            grid=(n_dev, inner),
            in_specs=[pl.BlockSpec((1, num_sent, step_rows, head_dim), lambda p, b, pos: (p, 0, b, 0)), cache_spec, cache_spec],
            out_specs=pl.BlockSpec((1, num_q, step_rows, head_dim), lambda p, b, pos: (p, 0, b, 0)),
            scratch_shapes=[
                pltpu.VMEM((step_rows * stride + 16, head_dim), jnp.float32),
                pltpu.VMEM((pad_q * (step_rows + 1) + 8, head_dim), jnp.float32),
            ],
        ),
        cost_estimate=pl.CostEstimate(flops=10**9, bytes_accessed=4 * k_own.size, transcendentals=0),
    )(start_pos, got, k_own, v_own)


def solution(mesh):
    n_dev = mesh.shape['x']
    row_spec = P(None, ('dp', 'x'), None)
    cache_in = P('dp', None, 'x', None)
    cache_out = P(('dp', 'x'), None, None, None)

    def local_run(start_pos, hidden_in, k_heads, v_heads, attn_norm, w_q, w_k, w_v, q_norm, k_norm, w_o, mlp_norm, w_gate, w_up, w_down):
        n_steps, num_rows, _ = hidden_in.shape
        _, num_slots, _, head_dim = k_heads.shape
        me = lax.axis_index('x')
        my_pos = lax.dynamic_slice_in_dim(start_pos, me * num_rows, num_rows)
        k_own, v_own = k_heads[:, :, 0], v_heads[:, :, 0]

        def swap(arr, rel_idx):
            return lax.ppermute(arr, 'x', [(d, d ^ rel_idx) for d in range(n_dev)])

        def swap_cache(own, row_base, chunk_rows):
            return [swap(lax.dynamic_slice_in_dim(own, jnp.bitwise_xor(me, rel_idx) * num_rows + row_base, chunk_rows), rel_idx) for rel_idx in SWAP_ORDER]

        cuts_k = cuts(num_rows, K_CUTS)
        positions = my_pos[None, :] + jnp.arange(n_steps)[:, None]
        queries, keys_new, values_new = project(hidden_in, positions, attn_norm, w_q, w_k, w_v, q_norm, k_norm)
        group = queries.shape[2] // n_dev
        q_send = queries.reshape(n_steps, num_rows, n_dev, group, head_dim).transpose(2, 0, 3, 1, 4).reshape(n_dev, n_steps * group, num_rows, head_dim)
        k_send = keys_new.transpose(2, 0, 1, 3)
        v_send = values_new.transpose(2, 0, 1, 3)
        sent = jnp.concatenate([q_send, k_send, v_send], axis=1)
        k_later, sent = lax.optimization_barrier((k_own, sent))
        k_got = [swap_cache(k_later if i else k_own, *c) for i, c in enumerate(cuts_k)]
        got = lax.all_to_all(sent, 'x', 0, 0, tiled=True)
        mixed = attend_local(got, k_own, v_own, start_pos, n_steps)
        v_got = lax.all_to_all(v_own, 'x', 0, 0, tiled=True).reshape(n_dev, num_rows, num_slots, head_dim)
        back = lax.all_to_all(mixed, 'x', 0, 0, tiled=True)
        attended = back.reshape(n_dev, n_steps, group, num_rows, head_dim).transpose(1, 3, 0, 2, 4).reshape(n_steps, num_rows, n_dev * group, head_dim)
        out_hidden = finish(hidden_in, attended, w_o, mlp_norm, w_gate, w_up, w_down)
        meta = jnp.concatenate([jnp.bitwise_xor(me, jnp.array((0,) + SWAP_ORDER)), my_pos]).astype(jnp.int32)
        k_out, v_out = None, merge_all(v_got, values_new, meta)
        for chunk_idx, ((row_base, chunk_rows), k_blocks) in enumerate(zip(cuts_k, k_got)):
            if chunk_idx == 2:
                meta, out_hidden = lax.optimization_barrier((meta, out_hidden))
            if chunk_idx == len(cuts_k) - 1:
                meta, v_out = lax.optimization_barrier((meta, v_out))
            k_out = merge_chunk(k_own, k_blocks, keys_new, meta, k_out, row_base, num_rows)
        return out_hidden, k_out, v_out

    return jax.shard_map(local_run, mesh=mesh, in_specs=(P('dp'), row_spec, cache_in, cache_in) + (P(),) * 11, out_specs=(row_spec, cache_out, cache_out), check_vma=False)
```

```python
import functools
import math

import jax
import jax.numpy as jnp
from jax import lax
from jax.experimental import pallas as pl
from jax.experimental.pallas import tpu as pltpu
from jax.sharding import PartitionSpec as P

EPS = 1e-6
THETA = 1000000.0


def rms_norm(values, gain_vec):
    values32 = values.astype(jnp.float32)
    inv_rms = lax.rsqrt(jnp.mean(values32 * values32, axis=-1, keepdims=True) + EPS)
    return values32 * inv_rms * gain_vec.astype(jnp.float32)


def rotary(values, positions):
    head_dim = values.shape[-1]
    half_dim = head_dim // 2
    inv_freq = jnp.power(THETA, -jnp.arange(half_dim, dtype=jnp.float32) * 2.0 / head_dim)
    angles = positions.astype(jnp.float32)[..., None, None] * inv_freq
    cos_part = jnp.cos(angles)
    sin_part = jnp.sin(angles)
    first_half = values[..., :half_dim]
    second_half = values[..., half_dim:]
    return jnp.concatenate([first_half * cos_part - second_half * sin_part, second_half * cos_part + first_half * sin_part], axis=-1)


def project(hidden, positions, attn_norm, w_q, w_k, w_v, q_norm, k_norm):
    n_steps, num_rows = hidden.shape[0], hidden.shape[1]
    head_dim = q_norm.shape[0]
    normed = rms_norm(hidden, attn_norm).astype(jnp.bfloat16)
    queries = jnp.einsum('sbd,de->sbe', normed, w_q, preferred_element_type=jnp.float32).reshape(n_steps, num_rows, -1, head_dim)
    keys_new = jnp.einsum('sbd,de->sbe', normed, w_k, preferred_element_type=jnp.float32).reshape(n_steps, num_rows, -1, head_dim)
    values_new = jnp.einsum('sbd,de->sbe', normed, w_v, preferred_element_type=jnp.float32).reshape(n_steps, num_rows, -1, head_dim)
    queries = rotary(rms_norm(queries, q_norm), positions).astype(jnp.bfloat16)
    keys_new = rotary(rms_norm(keys_new, k_norm), positions).astype(jnp.bfloat16)
    return queries, keys_new, values_new.astype(jnp.bfloat16)


def finish(hidden, attended, w_o, mlp_norm, w_gate, w_up, w_down):
    n_steps, num_rows = attended.shape[0], attended.shape[1]
    flat_attn = attended.reshape(n_steps, num_rows, -1)
    attn_out = jnp.einsum('sbe,ed->sbd', flat_attn, w_o, preferred_element_type=jnp.float32)
    residual = (hidden.astype(jnp.float32) + attn_out).astype(jnp.bfloat16)
    normed = rms_norm(residual, mlp_norm).astype(jnp.bfloat16)
    gate_val = jnp.einsum('sbd,df->sbf', normed, w_gate, preferred_element_type=jnp.float32)
    up_val = jnp.einsum('sbd,df->sbf', normed, w_up, preferred_element_type=jnp.float32)
    activated = (jax.nn.silu(gate_val) * up_val).astype(jnp.bfloat16)
    down_val = jnp.einsum('sbf,fd->sbd', activated, w_down, preferred_element_type=jnp.float32)
    return (residual.astype(jnp.float32) + down_val).astype(jnp.bfloat16)


ROW_PAD = 9
MERGE_ROWS = 4
ATTEND_ROWS = 8
K_CHUNKS = ((24, 8), (0, 20), (20, 4))
SWAP_ORDER = (2, 4, 3, 5, 6, 7, 1)


def merge_row(row_idx, block_refs, head_ids, fresh_ref, first_slot, out_ref, wide_ref):
    num_slots, n_dev = out_ref.shape[1], len(block_refs)
    for block_ref, head_idx in zip(block_refs, head_ids):
        wide_ref[pl.ds(head_idx, num_slots, stride=ROW_PAD), :] = block_ref[row_idx].astype(jnp.float32)
    for slot_idx in range(num_slots):
        out_ref[row_idx, slot_idx] = wide_ref[slot_idx * ROW_PAD:slot_idx * ROW_PAD + n_dev, :].astype(out_ref.dtype)
    for step_idx in range(fresh_ref.shape[0]):
        out_ref[row_idx, first_slot + step_idx] = fresh_ref[step_idx, row_idx]


def merge_chunk_kernel(row_base, n_dev, meta_ref, *refs):
    block_refs, fresh_ref, out_ref, wide_ref = refs[:n_dev], refs[n_dev], refs[-2], refs[-1]
    step_rows = out_ref.shape[0]
    head_ids = [meta_ref[rel_idx] for rel_idx in range(n_dev)]

    @pl.loop(0, step_rows)
    def _(row_idx):
        first_slot = meta_ref[n_dev + row_base + pl.program_id(0) * step_rows + row_idx]
        merge_row(row_idx, block_refs, head_ids, fresh_ref, first_slot, out_ref, wide_ref)


def merge_chunk(own, blocks, fresh_rows, meta, partial_out, row_base, num_rows):
    n_dev = len(blocks) + 1
    chunk_rows, num_slots, head_dim = blocks[0].shape
    n_steps = fresh_rows.shape[0]
    step_rows = math.gcd(math.gcd(chunk_rows, row_base), MERGE_ROWS)
    base = row_base // step_rows
    grid_spec = pltpu.PrefetchScalarGridSpec(
        num_scalar_prefetch=1,
        grid=(chunk_rows // step_rows,),
        in_specs=[pl.BlockSpec((step_rows, num_slots, head_dim), lambda b, meta: (meta[0] * (num_rows // step_rows) + base + b, 0, 0))]
        + [pl.BlockSpec((step_rows, num_slots, head_dim), lambda b, meta: (b, 0, 0))] * (n_dev - 1)
        + [pl.BlockSpec((n_steps, step_rows, n_dev, head_dim), lambda b, meta: (0, base + b, 0, 0))]
        + ([] if partial_out is None else [pl.BlockSpec(memory_space=pl.ANY)]),
        out_specs=pl.BlockSpec((step_rows, num_slots, n_dev, head_dim), lambda b, meta: (base + b, 0, 0, 0)),
        scratch_shapes=[pltpu.VMEM((num_slots * ROW_PAD, head_dim), jnp.float32)],
    )
    return pl.pallas_call(
        functools.partial(merge_chunk_kernel, row_base, n_dev),
        out_shape=jax.ShapeDtypeStruct((num_rows, num_slots, n_dev, head_dim), own.dtype),
        grid_spec=grid_spec,
        input_output_aliases={} if partial_out is None else {n_dev + 2: 0},
        cost_estimate=pl.CostEstimate(flops=10**8, bytes_accessed=4 * n_dev * blocks[0].size, transcendentals=0),
    )(meta, own, *blocks, fresh_rows, *(() if partial_out is None else (partial_out,)))


def merge_first_kernel(n_dev, meta_ref, blocks_ref, fresh_ref, partial_ref, out_ref, wide_ref):
    step_rows = out_ref.shape[0]

    @pl.loop(0, step_rows)
    def _(row_idx):
        first_slot = meta_ref[n_dev + pl.program_id(0) * step_rows + row_idx]
        merge_row(row_idx, [blocks_ref.at[h] for h in range(n_dev)], range(n_dev), fresh_ref, first_slot, out_ref, wide_ref)


def merge_first(blocks, fresh_rows, meta, partial_out):
    n_dev, chunk_rows, num_slots, head_dim = blocks.shape
    n_steps = fresh_rows.shape[0]
    step_rows = math.gcd(chunk_rows, 2 * MERGE_ROWS)
    return pl.pallas_call(
        functools.partial(merge_first_kernel, n_dev),
        out_shape=jax.ShapeDtypeStruct(partial_out.shape, blocks.dtype),
        grid_spec=pltpu.PrefetchScalarGridSpec(
            num_scalar_prefetch=1,
            grid=(chunk_rows // step_rows,),
            in_specs=[
                pl.BlockSpec((n_dev, step_rows, num_slots, head_dim), lambda b, meta: (0, b, 0, 0)),
                pl.BlockSpec((n_steps, step_rows, n_dev, head_dim), lambda b, meta: (0, b, 0, 0)),
                pl.BlockSpec(memory_space=pl.ANY),
            ],
            out_specs=pl.BlockSpec((step_rows, num_slots, n_dev, head_dim), lambda b, meta: (b, 0, 0, 0)),
            scratch_shapes=[pltpu.VMEM((num_slots * ROW_PAD, head_dim), jnp.float32)],
        ),
        input_output_aliases={3: 0},
        cost_estimate=pl.CostEstimate(flops=10**8, bytes_accessed=4 * blocks.size, transcendentals=0),
    )(meta, blocks, fresh_rows, partial_out)


def attend_kernel(n_steps, score_scale, meta_ref, sent_ref, k_ref, v_ref, out_ref, rows_ref, mixed_ref):
    num_sent, step_rows, head_dim = sent_ref.shape[1:]
    num_q = out_ref.shape[1]
    pad_q = num_sent + n_steps
    stride = num_sent + 1 - num_sent % 2
    group = num_q // n_steps
    num_slots = k_ref.shape[2]
    rows_ref[step_rows * stride:, :] = jnp.zeros((rows_ref.shape[0] - step_rows * stride, head_dim), jnp.float32)
    for sent_idx in range(num_sent):
        rows_ref[pl.ds(sent_idx, step_rows, stride=stride), :] = sent_ref[0, sent_idx].astype(jnp.float32)
    rows_ref[pl.ds(num_sent, step_rows, stride=stride), :] = jnp.zeros((step_rows, head_dim), jnp.float32)
    row_step = lax.broadcasted_iota(jnp.int32, (pad_q, pad_q), 0) // group
    col_step = lax.broadcasted_iota(jnp.int32, (pad_q, pad_q), 1) - num_q
    new_valid = (col_step >= 0) & (col_step < n_steps) & (col_step <= row_step)
    slot_ids = lax.broadcasted_iota(jnp.int32, (pad_q, num_slots), 1)
    over_lanes = (((1,), (1,)), ((), ()))
    base = pl.num_programs(0) + pl.program_id(0) * step_rows
    for first_row in range(0, step_rows, ATTEND_ROWS):
        rows = range(first_row, min(first_row + ATTEND_ROWS, step_rows))
        queries = [rows_ref[r * stride:r * stride + pad_q, :].astype(jnp.bfloat16) for r in rows]
        old = [lax.dot_general(q, k_ref[0, r], over_lanes, preferred_element_type=jnp.float32) for r, q in zip(rows, queries)]
        new = [lax.dot_general(q, q, over_lanes, preferred_element_type=jnp.float32) for q in queries]
        old = [jnp.where(slot_ids < meta_ref[base + r], s * score_scale, -jnp.inf) for r, s in zip(rows, old)]
        new = [jnp.where(new_valid, s * score_scale, -jnp.inf) for s in new]
        peak = [jnp.maximum(jnp.max(a, axis=-1, keepdims=True), jnp.max(c, axis=-1, keepdims=True)) for a, c in zip(old, new)]
        old = [jnp.exp(s - m) for s, m in zip(old, peak)]
        new = [jnp.exp(s - m) for s, m in zip(new, peak)]
        weight_sum = [jnp.sum(a, axis=-1, keepdims=True) + jnp.sum(c, axis=-1, keepdims=True) for a, c in zip(old, new)]
        mixed = [jnp.dot(w.astype(jnp.bfloat16), v_ref[0, r], preferred_element_type=jnp.float32) for r, w in zip(rows, old)]
        values_new = [rows_ref[r * stride + n_steps:r * stride + n_steps + pad_q, :].astype(jnp.bfloat16) for r in rows]
        fresh = [jnp.dot(w.astype(jnp.bfloat16), v, preferred_element_type=jnp.float32) for w, v in zip(new, values_new)]
        mixed = [(a + c) / s for a, c, s in zip(mixed, fresh, weight_sum)]
        for r, o in zip(rows, mixed):
            mixed_ref[pl.ds(r, pad_q, stride=step_rows + 1), :] = o
    for q_idx in range(num_q):
        at = q_idx * (step_rows + 1)
        out_ref[0, q_idx] = mixed_ref[at:at + step_rows, :].astype(out_ref.dtype)


def attend_local(sent, k_blocks, v_blocks, block_ids, first_slots, row_block, n_steps):
    n_dev, num_sent, _, head_dim = sent.shape
    step_rows = first_slots.shape[1]
    num_slots = k_blocks.shape[2]
    num_q = num_sent - 2 * n_steps
    pad_q = num_sent + n_steps
    stride = num_sent + 1 - num_sent % 2
    cache_spec = pl.BlockSpec((1, step_rows, num_slots, head_dim), lambda p, meta: (p, 0, 0, 0))
    return pl.pallas_call(
        functools.partial(attend_kernel, n_steps, head_dim ** -0.5),
        out_shape=jax.ShapeDtypeStruct((n_dev, num_q, step_rows, head_dim), sent.dtype),
        grid_spec=pltpu.PrefetchScalarGridSpec(
            num_scalar_prefetch=1,
            grid=(n_dev,),
            in_specs=[pl.BlockSpec((1, num_sent, step_rows, head_dim), lambda p, meta: (meta[p], 0, row_block, 0)), cache_spec, cache_spec],
            out_specs=pl.BlockSpec((1, num_q, step_rows, head_dim), lambda p, meta: (meta[p], 0, 0, 0)),
            scratch_shapes=[
                pltpu.VMEM((step_rows * stride + 16, head_dim), jnp.float32),
                pltpu.VMEM((pad_q * (step_rows + 1) + 8, head_dim), jnp.float32),
            ],
        ),
        cost_estimate=pl.CostEstimate(flops=10**9, bytes_accessed=4 * n_dev * step_rows * num_slots * head_dim, transcendentals=0),
    )(jnp.concatenate([block_ids, first_slots.reshape(-1)]).astype(jnp.int32), sent, k_blocks, v_blocks)


def solution(mesh):
    n_dev = mesh.shape['x']
    row_spec = P(None, ('dp', 'x'), None)
    cache_in = P('dp', None, 'x', None)
    cache_out = P(('dp', 'x'), None, None, None)

    def local_run(start_pos, hidden_in, k_heads, v_heads, attn_norm, w_q, w_k, w_v, q_norm, k_norm, w_o, mlp_norm, w_gate, w_up, w_down):
        n_steps, num_rows, _ = hidden_in.shape
        _, num_slots, _, head_dim = k_heads.shape
        me = lax.axis_index('x')
        my_pos = lax.dynamic_slice_in_dim(start_pos, me * num_rows, num_rows)
        k_own, v_own = k_heads[:, :, 0], v_heads[:, :, 0]

        def swap(arr, rel_idx):
            return lax.ppermute(arr, 'x', [(d, d ^ rel_idx) for d in range(n_dev)])

        def swap_cache(own, row_base, chunk_rows):
            return [swap(lax.dynamic_slice_in_dim(own, jnp.bitwise_xor(me, rel_idx) * num_rows + row_base, chunk_rows), rel_idx) for rel_idx in SWAP_ORDER]

        cuts_k = [(lo * num_rows // 32, n * num_rows // 32) for lo, n in K_CHUNKS]
        far_rows, near_rows = cuts_k[0]
        positions = my_pos[None, :] + jnp.arange(n_steps)[:, None]
        queries, keys_new, values_new = project(hidden_in, positions, attn_norm, w_q, w_k, w_v, q_norm, k_norm)
        group = queries.shape[2] // n_dev
        q_send = queries.reshape(n_steps, num_rows, n_dev, group, head_dim).transpose(2, 0, 3, 1, 4).reshape(n_dev, n_steps * group, num_rows, head_dim)
        k_send = keys_new.transpose(2, 0, 1, 3)
        v_send = values_new.transpose(2, 0, 1, 3)
        sent = jnp.concatenate([q_send, k_send, v_send], axis=1)
        k_later, v_later, sent = lax.optimization_barrier((k_own, v_own, sent))
        k_got = [swap_cache(k_later if i else k_own, *c) for i, c in enumerate(cuts_k)]
        v_near = swap_cache(v_later, far_rows, near_rows)
        got = lax.all_to_all(sent[:, :, :far_rows], 'x', 0, 0, tiled=True)
        peers = jnp.arange(n_dev, dtype=jnp.int32)
        by_peer = (n_dev, num_rows, num_slots, head_dim)
        mixed = attend_local(got, k_own.reshape(by_peer), v_own.reshape(by_peer), peers, start_pos.reshape(n_dev, num_rows)[:, :far_rows], 0, n_steps)
        v_got = lax.all_to_all(v_later.reshape(by_peer)[:, :far_rows], 'x', 0, 0, tiled=True)
        back = lax.all_to_all(mixed, 'x', 0, 0, tiled=True)
        head_ids = jnp.bitwise_xor(me, jnp.array((0,) + SWAP_ORDER, dtype=jnp.int32))
        k_near, v_near_late, _ = lax.optimization_barrier((k_got[0], v_near, mixed))
        near = [jnp.stack([lax.dynamic_slice_in_dim(own, me * num_rows + far_rows, near_rows)] + blocks) for own, blocks in ((k_later, k_near), (v_later, v_near_late))]
        mixed_near = attend_local(sent, *near, head_ids, jnp.broadcast_to(my_pos[far_rows:], (n_dev, near_rows)), far_rows // near_rows, n_steps)
        attended = jnp.concatenate([back, mixed_near], axis=2)
        attended = attended.reshape(n_dev, n_steps, group, num_rows, head_dim).transpose(1, 3, 0, 2, 4).reshape(n_steps, num_rows, n_dev * group, head_dim)
        out_hidden = finish(hidden_in, attended, w_o, mlp_norm, w_gate, w_up, w_down)
        meta = jnp.concatenate([head_ids, my_pos]).astype(jnp.int32)
        k_out = merge_chunk(k_own, k_got[0], keys_new, meta, None, *cuts_k[0][:1], num_rows)
        v_out = merge_chunk(v_own, v_near, values_new, meta, None, *cuts_k[0][:1], num_rows)
        meta, out_hidden = lax.optimization_barrier((meta, out_hidden))
        k_out = merge_chunk(k_own, k_got[1], keys_new, meta, k_out, cuts_k[1][0], num_rows)
        v_out = merge_first(v_got, values_new, meta, v_out)
        meta, v_out = lax.optimization_barrier((meta, v_out))
        k_out = merge_chunk(k_own, k_got[2], keys_new, meta, k_out, cuts_k[2][0], num_rows)
        return out_hidden, k_out, v_out

    return jax.shard_map(local_run, mesh=mesh, in_specs=(P('dp'), row_spec, cache_in, cache_in) + (P(),) * 11, out_specs=(row_spec, cache_out, cache_out), check_vma=False)
```

```python
import functools
import math

import jax
import jax.numpy as jnp
from jax import lax
from jax.experimental import pallas as pl
from jax.experimental.pallas import tpu as pltpu
from jax.sharding import PartitionSpec as P

EPS = 1e-6
THETA = 1000000.0


def rms_norm(values, gain_vec):
    values32 = values.astype(jnp.float32)
    inv_rms = lax.rsqrt(jnp.mean(values32 * values32, axis=-1, keepdims=True) + EPS)
    return values32 * inv_rms * gain_vec.astype(jnp.float32)


def rotary(values, positions):
    head_dim = values.shape[-1]
    half_dim = head_dim // 2
    inv_freq = jnp.power(THETA, -jnp.arange(half_dim, dtype=jnp.float32) * 2.0 / head_dim)
    angles = positions.astype(jnp.float32)[..., None, None] * inv_freq
    cos_part = jnp.cos(angles)
    sin_part = jnp.sin(angles)
    first_half = values[..., :half_dim]
    second_half = values[..., half_dim:]
    return jnp.concatenate([first_half * cos_part - second_half * sin_part, second_half * cos_part + first_half * sin_part], axis=-1)


def project(hidden, positions, attn_norm, w_q, w_k, w_v, q_norm, k_norm):
    n_steps, num_rows = hidden.shape[0], hidden.shape[1]
    head_dim = q_norm.shape[0]
    normed = rms_norm(hidden, attn_norm).astype(jnp.bfloat16)
    queries = jnp.einsum('sbd,de->sbe', normed, w_q, preferred_element_type=jnp.float32).reshape(n_steps, num_rows, -1, head_dim)
    keys_new = jnp.einsum('sbd,de->sbe', normed, w_k, preferred_element_type=jnp.float32).reshape(n_steps, num_rows, -1, head_dim)
    values_new = jnp.einsum('sbd,de->sbe', normed, w_v, preferred_element_type=jnp.float32).reshape(n_steps, num_rows, -1, head_dim)
    queries = rotary(rms_norm(queries, q_norm), positions).astype(jnp.bfloat16)
    keys_new = rotary(rms_norm(keys_new, k_norm), positions).astype(jnp.bfloat16)
    return queries, keys_new, values_new.astype(jnp.bfloat16)


def finish(hidden, attended, w_o, mlp_norm, w_gate, w_up, w_down):
    n_steps, num_rows = attended.shape[0], attended.shape[1]
    flat_attn = attended.reshape(n_steps, num_rows, -1)
    attn_out = jnp.einsum('sbe,ed->sbd', flat_attn, w_o, preferred_element_type=jnp.float32)
    residual = (hidden.astype(jnp.float32) + attn_out).astype(jnp.bfloat16)
    normed = rms_norm(residual, mlp_norm).astype(jnp.bfloat16)
    gate_val = jnp.einsum('sbd,df->sbf', normed, w_gate, preferred_element_type=jnp.float32)
    up_val = jnp.einsum('sbd,df->sbf', normed, w_up, preferred_element_type=jnp.float32)
    activated = (jax.nn.silu(gate_val) * up_val).astype(jnp.bfloat16)
    down_val = jnp.einsum('sbf,fd->sbd', activated, w_down, preferred_element_type=jnp.float32)
    return (residual.astype(jnp.float32) + down_val).astype(jnp.bfloat16)


ROW_PAD = 9
MERGE_ROWS = 4
ATTEND_ROWS = 8
K_CHUNKS = ((24, 8), (0, 20), (20, 4))
SWAP_ORDER = (2, 4, 3, 5, 6, 7, 1)


def merge_row(row_idx, block_refs, head_ids, fresh_ref, first_slot, out_ref, wide_ref):
    num_slots, n_dev = out_ref.shape[1], len(block_refs)
    for block_ref, head_idx in zip(block_refs, head_ids):
        wide_ref[pl.ds(head_idx, num_slots, stride=ROW_PAD), :] = block_ref[row_idx].astype(jnp.float32)
    for slot_idx in range(num_slots):
        out_ref[row_idx, slot_idx] = wide_ref[slot_idx * ROW_PAD:slot_idx * ROW_PAD + n_dev, :].astype(out_ref.dtype)
    for step_idx in range(fresh_ref.shape[0]):
        out_ref[row_idx, first_slot + step_idx] = fresh_ref[step_idx, row_idx]


def merge_chunk_kernel(row_base, n_dev, meta_ref, *refs):
    block_refs, fresh_ref, out_ref, wide_ref = refs[:n_dev], refs[n_dev], refs[-2], refs[-1]
    step_rows = out_ref.shape[0]
    head_ids = [meta_ref[rel_idx] for rel_idx in range(n_dev)]

    @pl.loop(0, step_rows)
    def _(row_idx):
        first_slot = meta_ref[n_dev + row_base + pl.program_id(0) * step_rows + row_idx]
        merge_row(row_idx, block_refs, head_ids, fresh_ref, first_slot, out_ref, wide_ref)


def merge_chunk(own, blocks, fresh_rows, meta, partial_out, row_base, num_rows):
    n_dev = len(blocks) + 1
    chunk_rows, num_slots, head_dim = blocks[0].shape
    n_steps = fresh_rows.shape[0]
    step_rows = math.gcd(math.gcd(chunk_rows, row_base), MERGE_ROWS)
    base = row_base // step_rows
    grid_spec = pltpu.PrefetchScalarGridSpec(
        num_scalar_prefetch=1,
        grid=(chunk_rows // step_rows,),
        in_specs=[pl.BlockSpec((step_rows, num_slots, head_dim), lambda b, meta: (meta[0] * (num_rows // step_rows) + base + b, 0, 0))]
        + [pl.BlockSpec((step_rows, num_slots, head_dim), lambda b, meta: (b, 0, 0))] * (n_dev - 1)
        + [pl.BlockSpec((n_steps, step_rows, n_dev, head_dim), lambda b, meta: (0, base + b, 0, 0))]
        + ([] if partial_out is None else [pl.BlockSpec(memory_space=pl.ANY)]),
        out_specs=pl.BlockSpec((step_rows, num_slots, n_dev, head_dim), lambda b, meta: (base + b, 0, 0, 0)),
        scratch_shapes=[pltpu.VMEM((num_slots * ROW_PAD, head_dim), jnp.float32)],
    )
    return pl.pallas_call(
        functools.partial(merge_chunk_kernel, row_base, n_dev),
        out_shape=jax.ShapeDtypeStruct((num_rows, num_slots, n_dev, head_dim), own.dtype),
        grid_spec=grid_spec,
        input_output_aliases={} if partial_out is None else {n_dev + 2: 0},
        cost_estimate=pl.CostEstimate(flops=10**8, bytes_accessed=4 * n_dev * blocks[0].size, transcendentals=0),
    )(meta, own, *blocks, fresh_rows, *(() if partial_out is None else (partial_out,)))


def merge_first_kernel(n_dev, meta_ref, blocks_ref, fresh_ref, partial_ref, out_ref, wide_ref):
    step_rows = out_ref.shape[0]

    @pl.loop(0, step_rows)
    def _(row_idx):
        first_slot = meta_ref[n_dev + pl.program_id(0) * step_rows + row_idx]
        merge_row(row_idx, [blocks_ref.at[h] for h in range(n_dev)], range(n_dev), fresh_ref, first_slot, out_ref, wide_ref)


def merge_first(blocks, fresh_rows, meta, partial_out):
    n_dev, chunk_rows, num_slots, head_dim = blocks.shape
    n_steps = fresh_rows.shape[0]
    step_rows = math.gcd(chunk_rows, 2 * MERGE_ROWS)
    return pl.pallas_call(
        functools.partial(merge_first_kernel, n_dev),
        out_shape=jax.ShapeDtypeStruct(partial_out.shape, blocks.dtype),
        grid_spec=pltpu.PrefetchScalarGridSpec(
            num_scalar_prefetch=1,
            grid=(chunk_rows // step_rows,),
            in_specs=[
                pl.BlockSpec((n_dev, step_rows, num_slots, head_dim), lambda b, meta: (0, b, 0, 0)),
                pl.BlockSpec((n_steps, step_rows, n_dev, head_dim), lambda b, meta: (0, b, 0, 0)),
                pl.BlockSpec(memory_space=pl.ANY),
            ],
            out_specs=pl.BlockSpec((step_rows, num_slots, n_dev, head_dim), lambda b, meta: (b, 0, 0, 0)),
            scratch_shapes=[pltpu.VMEM((num_slots * ROW_PAD, head_dim), jnp.float32)],
        ),
        input_output_aliases={3: 0},
        cost_estimate=pl.CostEstimate(flops=10**8, bytes_accessed=4 * blocks.size, transcendentals=0),
    )(meta, blocks, fresh_rows, partial_out)


def attend_kernel(n_steps, score_scale, meta_ref, sent_ref, k_ref, v_ref, out_ref, rows_ref, mixed_ref):
    num_sent, step_rows, head_dim = sent_ref.shape[1:]
    num_q = out_ref.shape[1]
    pad_q = num_sent + n_steps
    stride = num_sent + 1 - num_sent % 2
    group = num_q // n_steps
    num_slots = k_ref.shape[2]
    rows_ref[step_rows * stride:, :] = jnp.zeros((rows_ref.shape[0] - step_rows * stride, head_dim), jnp.float32)
    for sent_idx in range(num_sent):
        rows_ref[pl.ds(sent_idx, step_rows, stride=stride), :] = sent_ref[0, sent_idx].astype(jnp.float32)
    rows_ref[pl.ds(num_sent, step_rows, stride=stride), :] = jnp.zeros((step_rows, head_dim), jnp.float32)
    row_step = lax.broadcasted_iota(jnp.int32, (pad_q, pad_q), 0) // group
    col_step = lax.broadcasted_iota(jnp.int32, (pad_q, pad_q), 1) - num_q
    new_valid = (col_step >= 0) & (col_step < n_steps) & (col_step <= row_step)
    slot_ids = lax.broadcasted_iota(jnp.int32, (pad_q, num_slots), 1)
    over_lanes = (((1,), (1,)), ((), ()))
    base = pl.num_programs(0) + pl.program_id(0) * step_rows
    for first_row in range(0, step_rows, ATTEND_ROWS):
        rows = range(first_row, min(first_row + ATTEND_ROWS, step_rows))
        queries = [rows_ref[r * stride:r * stride + pad_q, :].astype(jnp.bfloat16) for r in rows]
        old = [lax.dot_general(q, k_ref[0, r], over_lanes, preferred_element_type=jnp.float32) for r, q in zip(rows, queries)]
        new = [lax.dot_general(q, q, over_lanes, preferred_element_type=jnp.float32) for q in queries]
        old = [jnp.where(slot_ids < meta_ref[base + r], s * score_scale, -jnp.inf) for r, s in zip(rows, old)]
        new = [jnp.where(new_valid, s * score_scale, -jnp.inf) for s in new]
        peak = [jnp.maximum(jnp.max(a, axis=-1, keepdims=True), jnp.max(c, axis=-1, keepdims=True)) for a, c in zip(old, new)]
        old = [jnp.exp(s - m) for s, m in zip(old, peak)]
        new = [jnp.exp(s - m) for s, m in zip(new, peak)]
        weight_sum = [jnp.sum(a, axis=-1, keepdims=True) + jnp.sum(c, axis=-1, keepdims=True) for a, c in zip(old, new)]
        mixed = [jnp.dot(w.astype(jnp.bfloat16), v_ref[0, r], preferred_element_type=jnp.float32) for r, w in zip(rows, old)]
        values_new = [rows_ref[r * stride + n_steps:r * stride + n_steps + pad_q, :].astype(jnp.bfloat16) for r in rows]
        fresh = [jnp.dot(w.astype(jnp.bfloat16), v, preferred_element_type=jnp.float32) for w, v in zip(new, values_new)]
        mixed = [(a + c) / s for a, c, s in zip(mixed, fresh, weight_sum)]
        for r, o in zip(rows, mixed):
            mixed_ref[pl.ds(r, pad_q, stride=step_rows + 1), :] = o
    for q_idx in range(num_q):
        at = q_idx * (step_rows + 1)
        out_ref[0, q_idx] = mixed_ref[at:at + step_rows, :].astype(out_ref.dtype)


def attend_local(sent, k_blocks, v_blocks, block_ids, first_slots, n_steps):
    n_dev, num_sent, _, head_dim = sent.shape
    step_rows = first_slots.shape[1]
    num_slots = k_blocks.shape[2]
    num_q = num_sent - 2 * n_steps
    pad_q = num_sent + n_steps
    stride = num_sent + 1 - num_sent % 2
    cache_spec = pl.BlockSpec((1, step_rows, num_slots, head_dim), lambda p, meta: (p, 0, 0, 0))
    return pl.pallas_call(
        functools.partial(attend_kernel, n_steps, head_dim ** -0.5),
        out_shape=jax.ShapeDtypeStruct((n_dev, num_q, step_rows, head_dim), sent.dtype),
        grid_spec=pltpu.PrefetchScalarGridSpec(
            num_scalar_prefetch=1,
            grid=(n_dev,),
            in_specs=[pl.BlockSpec((1, num_sent, step_rows, head_dim), lambda p, meta: (meta[p], 0, 0, 0)), cache_spec, cache_spec],
            out_specs=pl.BlockSpec((1, num_q, step_rows, head_dim), lambda p, meta: (meta[p], 0, 0, 0)),
            scratch_shapes=[
                pltpu.VMEM((step_rows * stride + 16, head_dim), jnp.float32),
                pltpu.VMEM((pad_q * (step_rows + 1) + 8, head_dim), jnp.float32),
            ],
        ),
        cost_estimate=pl.CostEstimate(flops=10**9, bytes_accessed=4 * n_dev * step_rows * num_slots * head_dim, transcendentals=0),
    )(jnp.concatenate([block_ids, first_slots.reshape(-1)]).astype(jnp.int32), sent, k_blocks, v_blocks)


def attend_near_kernel(n_steps, score_scale, n_dev, first_row, num_rows, meta_ref, sent_ref, *refs):
    k_srcs, v_srcs = refs[:n_dev], refs[n_dev:2 * n_dev]
    out_ref, rows_ref, mixed_ref, k_buf, v_buf, copy_sems = refs[2 * n_dev:]
    near_rows = k_buf.shape[1]
    block_idx = pl.program_id(0)

    @pl.when(block_idx == 0)
    def _():
        own = pl.ds(meta_ref[0] * num_rows + first_row, near_rows)
        for rel_idx in range(n_dev):
            for kind, (srcs, buf) in enumerate(((k_srcs, k_buf), (v_srcs, v_buf))):
                src = srcs[rel_idx] if rel_idx else srcs[0].at[own]
                pltpu.make_async_copy(src, buf.at[rel_idx], copy_sems.at[kind, rel_idx]).start()

    for kind, (srcs, buf) in enumerate(((k_srcs, k_buf), (v_srcs, v_buf))):
        pltpu.make_async_copy(srcs[1], buf.at[block_idx], copy_sems.at[kind, block_idx]).wait()
    block = pl.ds(block_idx, 1)
    attend_kernel(n_steps, score_scale, meta_ref, sent_ref, k_buf.at[block], v_buf.at[block], out_ref, rows_ref, mixed_ref)


def attend_near(sent, k_blocks, v_blocks, block_ids, my_slots, first_row, n_steps):
    n_dev, num_sent, num_rows, head_dim = sent.shape
    near_rows, num_slots = k_blocks[1].shape[:2]
    num_q = num_sent - 2 * n_steps
    pad_q = num_sent + n_steps
    stride = num_sent + 1 - num_sent % 2
    first_slots = jnp.broadcast_to(my_slots, (n_dev, near_rows)).reshape(-1)
    return pl.pallas_call(
        functools.partial(attend_near_kernel, n_steps, head_dim ** -0.5, n_dev, first_row, num_rows),
        out_shape=jax.ShapeDtypeStruct((n_dev, num_q, near_rows, head_dim), sent.dtype),
        grid_spec=pltpu.PrefetchScalarGridSpec(
            num_scalar_prefetch=1,
            grid=(n_dev,),
            in_specs=[pl.BlockSpec((1, num_sent, near_rows, head_dim), lambda p, meta: (meta[p], 0, first_row // near_rows, 0))]
            + [pl.BlockSpec(memory_space=pl.ANY)] * (2 * n_dev),
            out_specs=pl.BlockSpec((1, num_q, near_rows, head_dim), lambda p, meta: (meta[p], 0, 0, 0)),
            scratch_shapes=[
                pltpu.VMEM((near_rows * stride + 16, head_dim), jnp.float32),
                pltpu.VMEM((pad_q * (near_rows + 1) + 8, head_dim), jnp.float32),
                pltpu.VMEM((n_dev, near_rows, num_slots, head_dim), sent.dtype),
                pltpu.VMEM((n_dev, near_rows, num_slots, head_dim), sent.dtype),
                pltpu.SemaphoreType.DMA((2, n_dev)),
            ],
        ),
        cost_estimate=pl.CostEstimate(flops=10**9, bytes_accessed=4 * n_dev * near_rows * num_slots * head_dim, transcendentals=0),
    )(jnp.concatenate([block_ids, first_slots]).astype(jnp.int32), sent, *k_blocks, *v_blocks)


def solution(mesh):
    n_dev = mesh.shape['x']
    row_spec = P(None, ('dp', 'x'), None)
    cache_in = P('dp', None, 'x', None)
    cache_out = P(('dp', 'x'), None, None, None)

    def local_run(start_pos, hidden_in, k_heads, v_heads, attn_norm, w_q, w_k, w_v, q_norm, k_norm, w_o, mlp_norm, w_gate, w_up, w_down):
        n_steps, num_rows, _ = hidden_in.shape
        _, num_slots, _, head_dim = k_heads.shape
        me = lax.axis_index('x')
        my_pos = lax.dynamic_slice_in_dim(start_pos, me * num_rows, num_rows)
        k_own, v_own = k_heads[:, :, 0], v_heads[:, :, 0]

        def swap(arr, rel_idx):
            return lax.ppermute(arr, 'x', [(d, d ^ rel_idx) for d in range(n_dev)])

        def swap_cache(own, row_base, chunk_rows):
            return [swap(lax.dynamic_slice_in_dim(own, jnp.bitwise_xor(me, rel_idx) * num_rows + row_base, chunk_rows), rel_idx) for rel_idx in SWAP_ORDER]

        cuts_k = [(lo * num_rows // 32, n * num_rows // 32) for lo, n in K_CHUNKS]
        far_rows, near_rows = cuts_k[0]
        positions = my_pos[None, :] + jnp.arange(n_steps)[:, None]
        queries, keys_new, values_new = project(hidden_in, positions, attn_norm, w_q, w_k, w_v, q_norm, k_norm)
        group = queries.shape[2] // n_dev
        q_send = queries.reshape(n_steps, num_rows, n_dev, group, head_dim).transpose(2, 0, 3, 1, 4).reshape(n_dev, n_steps * group, num_rows, head_dim)
        k_send = keys_new.transpose(2, 0, 1, 3)
        v_send = values_new.transpose(2, 0, 1, 3)
        sent = jnp.concatenate([q_send, k_send, v_send], axis=1)
        k_later, v_later, sent = lax.optimization_barrier((k_own, v_own, sent))
        k_got = [swap_cache(k_later if i else k_own, *c) for i, c in enumerate(cuts_k)]
        v_near = swap_cache(v_later, far_rows, near_rows)
        got = lax.all_to_all(sent[:, :, :far_rows], 'x', 0, 0, tiled=True)
        peers = jnp.arange(n_dev, dtype=jnp.int32)
        by_peer = (n_dev, num_rows, num_slots, head_dim)
        mixed = attend_local(got, k_own.reshape(by_peer), v_own.reshape(by_peer), peers, start_pos.reshape(n_dev, num_rows)[:, :far_rows], n_steps)
        v_got = lax.all_to_all(v_later.reshape(by_peer)[:, :far_rows], 'x', 0, 0, tiled=True)
        back = lax.all_to_all(mixed, 'x', 0, 0, tiled=True)
        head_ids = jnp.bitwise_xor(me, jnp.array((0,) + SWAP_ORDER, dtype=jnp.int32))
        mixed_near = attend_near(sent, [k_own] + k_got[0], [v_own] + v_near, head_ids, my_pos[far_rows:], far_rows, n_steps)
        attended = jnp.concatenate([back, mixed_near], axis=2)
        attended = attended.reshape(n_dev, n_steps, group, num_rows, head_dim).transpose(1, 3, 0, 2, 4).reshape(n_steps, num_rows, n_dev * group, head_dim)
        out_hidden = finish(hidden_in, attended, w_o, mlp_norm, w_gate, w_up, w_down)
        meta = jnp.concatenate([head_ids, my_pos]).astype(jnp.int32)
        k_out = merge_chunk(k_own, k_got[0], keys_new, meta, None, *cuts_k[0][:1], num_rows)
        v_out = merge_chunk(v_own, v_near, values_new, meta, None, *cuts_k[0][:1], num_rows)
        meta, out_hidden = lax.optimization_barrier((meta, out_hidden))
        k_out = merge_chunk(k_own, k_got[1], keys_new, meta, k_out, cuts_k[1][0], num_rows)
        v_out = merge_first(v_got, values_new, meta, v_out)
        meta, v_out = lax.optimization_barrier((meta, v_out))
        k_out = merge_chunk(k_own, k_got[2], keys_new, meta, k_out, cuts_k[2][0], num_rows)
        return out_hidden, k_out, v_out

    return jax.shard_map(local_run, mesh=mesh, in_specs=(P('dp'), row_spec, cache_in, cache_in) + (P(),) * 11, out_specs=(row_spec, cache_out, cache_out), check_vma=False)
```
